16 devices in a mesh: dp: 2 (over y, z), tp: 8 (over x, core).
Axes of the slice: x: 4, y: 2, z: 1, core: 2. Of those that a mesh axis runs over, the one named last changes fastest.
The devices are a block of a 4x4x8 slice.
Arguments:
- ids: int32 [4, 256], P('dp'), parts along dimension 0
- emb: bfloat16 [65536, 2048], P('tp')
- g: bfloat16 [2048], replicated
- w: bfloat16 [2048, 3072], P(None, 'tp')
- du: bfloat16 [4, 256, 3072], P('dp', None, 'tp'), parts along dimension 0
- dres: bfloat16 [4, 256, 2048], P('dp', 'tp'), parts along dimension 0
Outputs:
- output 1: bfloat16 [4, 256, 3072], P('dp', None, 'tp'), parts along dimension 0
- output 2: bfloat16 [4, 256, 2048], P('dp', 'tp'), parts along dimension 0
- output 3: float32 [131072, 2048], P(('dp', 'tp')), parts along dimension 0
- output 4: float32 [2048, 6144], P(None, ('dp', 'tp')), parts along dimension 1
- output 5: float32 [4096], P('dp'), parts along dimension 0
There are 2 independent parts. The reference program is written for one: setup_inputs(seed, part) draws one part's arguments, and reference() takes and returns one part's arrays. A program takes and returns all parts, laid end to end along the dimension named above; an argument that names none is the same for every part.
All inputs are finite; a program needn't handle non-finite values.
Results may differ from the reference program's by a relative error of at most 0.001.
Values are sent between devices in bfloat16 or wider.
A program may use at most 768 MiB of HBM per device.

```python
import jax
import jax.numpy as jnp
from jax import lax

K = 2
T = 256
V = 65536
D = 2048
FC = 3072
GROUP = 8
EPS = 1e-6
NPOOL = K * T // 16
FCG = FC // GROUP


def setup_inputs(seed: int = 0, part: int = 0) -> dict:
    key = jax.random.key(seed)
    kp = jax.random.fold_in(key, part)
    ke, kg, kw = jax.random.split(key, 3)
    k1, k2, k3, k4, k5, k6 = jax.random.split(kp, 6)
    ka, kb, kc = jax.random.split(jax.random.fold_in(kp, 7), 3)
    a = jax.random.randint(ka, (K, T), 0, V)
    b = jax.random.randint(kb, (K, T), 0, V)
    coin = jax.random.bernoulli(kc, 0.4, (K, T))
    ids = jnp.where(coin, a, jnp.minimum(a, b)).astype(jnp.int32)
    emb = jax.random.normal(ke, (V, D), jnp.float32).astype(jnp.bfloat16)
    g = (1.0 + 0.5 * jax.random.normal(kg, (D,), jnp.float32)).astype(jnp.bfloat16)
    w = (jax.random.normal(kw, (D, FC), jnp.float32) * D ** -0.5).astype(jnp.bfloat16)
    du = (jax.random.normal(k5, (K, T, FC), jnp.float32) * (D / FC) ** 0.5).astype(jnp.bfloat16)
    dres = jax.random.normal(k6, (K, T, D), jnp.float32).astype(jnp.bfloat16)
    return {"ids": ids, "emb": emb, "g": g, "w": w, "du": du, "dres": dres}


def reference(ids, emb, g, w, du, dres):
    gf = g.astype(jnp.float32)

    def micro(carry, inp):
        de, dw, dg = carry
        idm, dum, drm = inp
        x = emb[idm]
        xf = x.astype(jnp.float32)
        rs = lax.rsqrt(jnp.mean(xf * xf, axis=-1, keepdims=True) + EPS)
        nh = xf * rs
        n = (nh * gf).astype(jnp.bfloat16)
        u = jnp.dot(n, w, preferred_element_type=jnp.float32).astype(jnp.bfloat16)
        dn = jnp.zeros((T, D), jnp.float32)
        for j in range(GROUP):
            pb = jnp.dot(dum[:, j * FCG:(j + 1) * FCG], w[:, j * FCG:(j + 1) * FCG].T, preferred_element_type=jnp.float32)
            dn = dn + pb.astype(jnp.bfloat16).astype(jnp.float32)
        gdn = gf * dn
        dxn = rs * (gdn - nh * jnp.mean(nh * gdn, axis=-1, keepdims=True))
        dx = (drm.astype(jnp.float32) + dxn).astype(jnp.bfloat16)
        de = de.at[idm].add(dx.astype(jnp.float32))
        dw = dw + jnp.dot(n.T, dum, preferred_element_type=jnp.float32)
        dg = dg + jnp.sum(dn * nh, axis=0)
        return (de, dw, dg), (u, x)

    init = (jnp.zeros((V, D), jnp.float32), jnp.zeros((D, FC), jnp.float32), jnp.zeros((D,), jnp.float32))
    (de, dw, dg), (u, x) = lax.scan(micro, init, (ids, du, dres))
    return u, x, de, dw, dg
```

```python
import functools

import jax
import jax.numpy as jnp
from jax import lax
from jax.experimental import pallas as pl
from jax.experimental.pallas import tpu as pltpu
from jax.sharding import PartitionSpec as P

EPS = 1e-6
MESH = pl.DeviceIdType.MESH
VMEM = pl.BlockSpec(memory_space=pltpu.VMEM)
SMEM = pl.BlockSpec(memory_space=pltpu.SMEM)
ANY = pl.BlockSpec(memory_space=pl.ANY)
F32 = jnp.float32
BF16 = jnp.bfloat16


def exchange(n, p_ref, du_ref, w_ref, g_ref, dres_ref, y_ref, dg_ref,
             d_s, prx, prd, sx, sd, rx, rd, nh_s, rs_s, dgs,
             pxs, pxr, pds, pdr, xs_sem, xr_sem, ds_sem, dr_sem, gs_sem, gr_sem):
    me = lax.axis_index("tp")
    chips = n // 2
    chip, core = me // 2, me % 2
    partner = chip * 2 + 1 - core
    right = ((chip + 1) % chips) * 2 + core
    left = ((chip + chips - 1) % chips) * 2 + core
    k, h, d = dres_ref.shape
    t = du_ref.shape[1]

    def dev(j, same):
        return ((chip + j) % chips) * 2 + (core if same else 1 - core)

    barrier = pltpu.get_barrier_semaphore()
    for o in range(1, n):
        pl.semaphore_signal(barrier, inc=1, device_id={"tp": (me + o) % n}, device_id_type=MESH)
    pl.semaphore_wait(barrier, n - 1)

    copies = []

    def send(src, dst, ss, rs, to):
        c = pltpu.make_async_remote_copy(src_ref=src, dst_ref=dst, send_sem=ss, recv_sem=rs,
                                         device_id={"tp": to}, device_id_type=MESH)
        c.start()
        copies.append(c)

    def arrived(dst, ss, rs):
        pltpu.make_async_remote_copy(src_ref=dst, dst_ref=dst, send_sem=ss, recv_sem=rs,
                                     device_id={"tp": partner}, device_id_type=MESH).wait_recv()

    order = (2, 1, 3, 0)
    for j in order:
        send(p_ref.at[dev(j, False)], prx.at[j], pxs.at[j], pxr.at[j], partner)

    def partial_dn(m):
        cw = 512

        def cols(i, _):
            c0 = pl.multiple_of(i * cw, cw)
            v = lax.dot_general(du_ref[m], w_ref[pl.ds(c0, cw), :], (((1,), (1,)), ((), ())),
                                preferred_element_type=F32)
            d_s[:, m * h:(m + 1) * h, pl.ds(c0, cw)] = v.astype(BF16).reshape(n, h, cw)
            return 0

        lax.fori_loop(0, d // cw, cols, 0)

    def half(ref, j, m):
        return ref.at[j, pl.ds(m * h, h)]

    def ring(s, r, ss, rs, direction, chunk, src):
        send(src, r.at[direction, chunk], ss.at[direction, chunk], rs.at[direction, chunk],
             right if direction == 0 else left)

    def first_hops(j, s, r, ss, rs):
        if j == 2:
            ring(s, r, ss, rs, 0, 0, half(s, 2, 0))
            ring(s, r, ss, rs, 1, 0, half(s, 2, 1))
        if j == 1:
            ring(s, r, ss, rs, 0, 1, half(s, 1, 1))
        if j == 3:
            ring(s, r, ss, rs, 1, 1, half(s, 3, 0))

    partial_dn(0)
    for j in order:
        arrived(prx.at[j], pxs.at[j], pxr.at[j])
        sx[j] = p_ref[dev(j, True)] + prx[j]
        first_hops(j, sx, rx, xs_sem, xr_sem)
    partial_dn(1)
    for j in order:
        send(d_s.at[dev(j, False)], prd.at[j], pds.at[j], pdr.at[j], partner)
    for j in order:
        arrived(prd.at[j], pds.at[j], pdr.at[j])
        sd[j] = d_s[dev(j, True)].astype(F32) + prd[j].astype(F32)
        first_hops(j, sd, rd, ds_sem, dr_sem)

    def second_hops(s, r, ss, rs):
        arrived(r.at[0, 0], ss.at[0, 0], rs.at[0, 0])
        s[1, :h] = s[1, :h] + r[0, 0]
        ring(s, r, ss, rs, 0, 2, half(s, 1, 0))
        arrived(r.at[1, 0], ss.at[1, 0], rs.at[1, 0])
        s[3, h:] = s[3, h:] + r[1, 0]
        ring(s, r, ss, rs, 1, 2, half(s, 3, 1))

    second_hops(sx, rx, xs_sem, xr_sem)
    second_hops(sd, rd, ds_sem, dr_sem)

    q = 16
    steps = h // q
    for dr, c in ((0, 1), (1, 1), (0, 2), (1, 2)):
        arrived(rx.at[dr, c], xs_sem.at[dr, c], xr_sem.at[dr, c])
    for m in range(k):
        ca, cb = (2, 1) if m == 0 else (1, 2)

        def norm(i, _):
            r0 = pl.multiple_of(i * q, q)
            rows = pl.ds(r0, q)
            x = sx[0, pl.ds(m * h + r0, q)] + rx[0, ca, rows] + rx[1, cb, rows]
            y_ref[0, m, rows] = x
            xf = x.astype(F32)
            rs = lax.rsqrt(jnp.mean(xf * xf, axis=-1, keepdims=True) + EPS)
            nh_s[m, rows] = xf * rs
            rs_s[m, rows] = jnp.broadcast_to(rs, (q, rs_s.shape[-1]))
            return 0

        lax.fori_loop(0, steps, norm, 0)

    for dr, c in ((0, 1), (1, 1), (0, 2), (1, 2)):
        arrived(rd.at[dr, c], ds_sem.at[dr, c], dr_sem.at[dr, c])
    dg = jnp.zeros((1, d), F32)
    for m in range(k):
        ca, cb = (2, 1) if m == 0 else (1, 2)

        def total(i, acc):
            r0 = pl.multiple_of(i * q, q)
            rows = pl.ds(r0, q)
            dn = sd[0, pl.ds(m * h + r0, q)] + rd[0, ca, rows] + rd[1, cb, rows]
            sd[0, pl.ds(m * h + r0, q)] = dn
            return acc + jnp.sum(dn * nh_s[m, rows], axis=0, keepdims=True)

        dg = lax.fori_loop(0, steps, total, dg)
    dgs[me] = dg
    for o in range(1, n):
        send(dgs.at[me], dgs.at[me], gs_sem.at[o], gr_sem.at[me], (me + o) % n)

    gf = g_ref[...].astype(F32)
    for m in range(k):
        def grad(i, _):
            r0 = pl.multiple_of(i * q, q)
            rows = pl.ds(r0, q)
            nh = nh_s[m, rows]
            gdn = gf * sd[0, pl.ds(m * h + r0, q)]
            dxn = rs_s[m, rows, :1] * (gdn - nh * jnp.mean(nh * gdn, axis=-1, keepdims=True))
            y_ref[1, m, rows] = (dres_ref[m, rows].astype(F32) + dxn).astype(BF16)
            return 0

        lax.fori_loop(0, steps, grad, 0)

    for o in range(1, n):
        src = (me + o) % n
        arrived(dgs.at[src], gs_sem.at[o], gr_sem.at[src])
    total_dg = dgs[0]
    for i in range(1, n):
        total_dg = total_dg + dgs[i]
    dg_ref[...] = total_dg
    for c in copies:
        c.wait_send()


def clear(first, rows, prev, tie_ref, z_in, de_ref, z, sem):
    del prev, tie_ref, z_in
    z[...] = jnp.zeros_like(z)
    zr = z.shape[0]
    cs = [pltpu.make_async_copy(z, de_ref.at[pl.ds(first + i * zr, zr)], sem) for i in range(rows // zr)]
    for c in cs:
        c.start()
    for c in cs:
        c.wait()


def clear_first(first, rows, tie_ref, de_ref, z, sem):
    clear(first, rows, None, tie_ref, None, de_ref, z, sem)


def clear_next(first, rows, tie_ref, z_in, de_ref, z, sem):
    clear(first, rows, None, tie_ref, z_in, de_ref, z, sem)


def finish(n, ids_ref, *refs):
    np_ = 2 * n
    xs, dxs = refs[:n], refs[n:np_]
    w_ref, du_ref, g_ref, de_in, u_ref, dw_ref, de_ref = refs[np_:np_ + 7]
    n_s, dxb, dxf, acc, table, blocks, sem = refs[np_ + 7:]
    del de_in
    me = lax.axis_index("tp")
    chips = n // 2
    chip, core = me // 2, me % 2
    k, h, d = xs[0].shape
    t = h * n
    vl = de_ref.shape[0] * de_ref.shape[1]
    lo = me * vl
    gf = g_ref[...].astype(F32)
    offs = (0, chips - 1, 1, 2)
    devs = [((chip + offs[i % 4]) % chips) * 2 + (core if i < 4 else 1 - core) for i in range(n)]
    q = 16
    for i in range(n):
        for m in range(k):
            def one(s, _):
                r0 = pl.multiple_of(s * q, q)
                rows = pl.ds(r0, q)
                xf = xs[i][m, rows].astype(F32)
                rs = lax.rsqrt(jnp.mean(xf * xf, axis=-1, keepdims=True) + EPS)
                n_s[pl.ds(pl.multiple_of(m * t + devs[i] * h + r0, q), q)] = ((xf * rs) * gf).astype(BF16)
                dxf[pl.ds(pl.multiple_of(devs[i] * (k * h) + m * h + r0, q), q)] = dxs[i][m, rows].astype(F32)
                return 0

            lax.fori_loop(0, h // q, one, 0)

    nb = table.shape[0]

    def reset(i, _):
        table[i] = -1
        return 0

    lax.fori_loop(0, nb, reset, 0, unroll=8)
    sub = lax.broadcasted_iota(jnp.int32, (8, d), 0)

    def scatter(i, cnt):
        v = ids_ref[i] - lo
        owned = (v >= 0) & (v < vl)

        def hit(cnt):
            b = v // 8
            slot0 = table[b]
            fresh = slot0 < 0
            slot = jnp.where(fresh, cnt, slot0)
            table[b] = slot
            blocks[slot] = b
            row = jnp.where(sub == v % 8, jnp.broadcast_to(dxf[pl.ds(i, 1)], (8, d)), 0.0)
            acc[slot] = row + jnp.where(fresh, jnp.zeros((8, d), F32), acc[slot])
            return jnp.where(fresh, cnt + 1, cnt)

        return lax.cond(owned, hit, lambda c: c, cnt)

    cnt = lax.fori_loop(0, k * t, scatter, 0)

    def put(i, _):
        pltpu.make_async_copy(acc.at[i], de_ref.at[blocks[i]], sem).start()
        return 0

    lax.fori_loop(0, cnt, put, 0)

    w = w_ref[...]
    for m in range(k):
        u_ref[m] = jnp.dot(n_s[m * t:(m + 1) * t], w, preferred_element_type=F32).astype(BF16)
    cw = 256

    def wgrad(i, _):
        c0 = pl.multiple_of(i * cw, cw)
        v = jnp.zeros((cw, w_ref.shape[1]), F32)
        for m in range(k):
            v = v + lax.dot_general(n_s[m * t:(m + 1) * t, pl.ds(c0, cw)], du_ref[m], (((0,), (0,)), ((), ())),
                                    preferred_element_type=F32)
        dw_ref[pl.ds(c0, cw)] = v
        return 0

    lax.fori_loop(0, d // cw, wgrad, 0)

    def drain(i, _):
        pltpu.make_async_copy(acc.at[i], de_ref.at[blocks[i]], sem).wait()
        return 0

    lax.fori_loop(0, cnt, drain, 0)


def solution(mesh):
    n = mesh.shape["tp"]
    chips = n // 2
    to_right = [(r, (r + 2) % n) for r in range(n)]
    to_left = [(r, (r + n - 2) % n) for r in range(n)]
    to_partner = [(r, r ^ 1) for r in range(n)]

    def local(ids, emb, g, w, du, dres):
        r = lax.axis_index("tp")
        k, t = ids.shape
        vl, d = emb.shape
        f = w.shape[1]
        h = t // n
        g2 = g.reshape(1, d)
        slab_ids = ids.reshape(k, n, h).transpose(1, 0, 2).reshape(-1)
        loc = slab_ids - r * vl
        own = (loc >= 0) & (loc < vl)
        rows = jnp.where(own[:, None], emb[jnp.clip(loc, 0, vl - 1)], jnp.zeros((), BF16))

        dma = pltpu.SemaphoreType.DMA
        y, dg = pl.pallas_call(
            functools.partial(exchange, n),
            out_shape=(jax.ShapeDtypeStruct((2, k, h, d), BF16), jax.ShapeDtypeStruct((1, d), F32)),
            in_specs=[VMEM] * 5,
            out_specs=(VMEM, VMEM),
            scratch_shapes=[
                pltpu.VMEM((n, k * h, d), BF16),
                pltpu.VMEM((chips, k * h, d), BF16),
                pltpu.VMEM((chips, k * h, d), BF16),
                pltpu.VMEM((chips, k * h, d), BF16),
                pltpu.VMEM((chips, k * h, d), F32),
                pltpu.VMEM((2, 3, h, d), BF16),
                pltpu.VMEM((2, 3, h, d), F32),
                pltpu.VMEM((k, h, d), F32),
                pltpu.VMEM((k, h, 128), F32),
                pltpu.VMEM((n, 1, d), F32),
                dma((chips,)), dma((chips,)), dma((chips,)), dma((chips,)),
                dma((2, 3)), dma((2, 3)), dma((2, 3)), dma((2, 3)),
                dma((n,)), dma((n,)),
            ],
            compiler_params=pltpu.CompilerParams(collective_id=0, has_side_effects=True, vmem_limit_bytes=40 << 20),
            name="exchange",
        )(rows.reshape(n, k * h, d), du, w, g2, dres)

        yl = lax.ppermute(y, "tp", to_right)
        yr = lax.ppermute(y, "tp", to_left)
        py = lax.ppermute(y, "tp", to_partner)
        xo = lax.ppermute(yl[0], "tp", to_right)
        do = lax.ppermute(yr[1], "tp", to_left)
        pyl = lax.ppermute(yl, "tp", to_partner)
        pyr = lax.ppermute(yr, "tp", to_partner)
        pxo = lax.ppermute(xo, "tp", to_partner)
        pdo = lax.ppermute(do, "tp", to_partner)

        zr = 512
        split = (vl * 5 // 8) // zr * zr
        zcost = lambda b: pl.CostEstimate(flops=0, bytes_accessed=b, transcendentals=0)
        de = pl.pallas_call(
            functools.partial(clear_first, 0, split),
            out_shape=jax.ShapeDtypeStruct((vl, d), F32),
            in_specs=[ANY], out_specs=ANY,
            scratch_shapes=[pltpu.VMEM((zr, d), F32), dma],
            cost_estimate=zcost(split * d * 4),
            name="clear0",
        )(dg)
        de = pl.pallas_call(
            functools.partial(clear_next, split, vl - split),
            out_shape=jax.ShapeDtypeStruct((vl, d), F32),
            in_specs=[ANY, ANY], out_specs=ANY,
            input_output_aliases={1: 0},
            scratch_shapes=[pltpu.VMEM((zr, d), F32), dma],
            cost_estimate=zcost((vl - split) * d * 4),
            name="clear1",
        )(yl, de)

        xs = [y[0], yl[0], yr[0], xo, py[0], pyl[0], pyr[0], pxo]
        dxs = [y[1], yl[1], yr[1], do, py[1], pyl[1], pyr[1], pdo]
        u, dw, de = pl.pallas_call(
            functools.partial(finish, n),
            out_shape=(jax.ShapeDtypeStruct((k, t, f), BF16), jax.ShapeDtypeStruct((d, f), F32),
                       jax.ShapeDtypeStruct((vl // 8, 8, d), F32)),
            in_specs=[SMEM] + [VMEM] * (2 * n + 3) + [ANY],
            out_specs=(VMEM, VMEM, ANY),
            input_output_aliases={2 * n + 4: 2},
            scratch_shapes=[
                pltpu.VMEM((k * t, d), BF16),
                pltpu.VMEM((8, d), BF16),
                pltpu.VMEM((k * t, d), F32),
                pltpu.VMEM((k * t, 8, d), F32),
                pltpu.SMEM((vl // 8,), jnp.int32),
                pltpu.SMEM((k * t,), jnp.int32),
                dma,
            ],
            compiler_params=pltpu.CompilerParams(vmem_limit_bytes=60 << 20),
            name="finish",
        )(slab_ids, *xs, *dxs, w, du, g2, de.reshape(vl // 8, 8, d))
        return u, y[0], de.reshape(vl, d), dw, dg.reshape(d)

    return jax.shard_map(
        local,
        mesh=mesh,
        in_specs=(P("dp", None), P("tp", None), P(None), P(None, "tp"), P("dp", None, "tp"), P("dp", "tp", None)),
        out_specs=(P("dp", None, "tp"), P("dp", "tp", None), P(("dp", "tp"), None), P(None, ("dp", "tp")), P("dp")),
        check_vma=False,
    )
```

```python
import functools

import jax
import jax.numpy as jnp
from jax import lax
from jax.experimental import pallas as pl
from jax.experimental.pallas import tpu as pltpu
from jax.sharding import PartitionSpec as P

EPS = 1e-6
MESH = pl.DeviceIdType.MESH
VMEM = pl.BlockSpec(memory_space=pltpu.VMEM)
SMEM = pl.BlockSpec(memory_space=pltpu.SMEM)
ANY = pl.BlockSpec(memory_space=pl.ANY)
F32 = jnp.float32
BF16 = jnp.bfloat16
ROWS = 16
SLOTS = 128


def lookup(n, ids_ref, emb_ref, du_hbm, w_hbm, p_ref, d_ref, at_ref, row_ref, count_ref,
           du_s, w_s, buf, pf, sem, in_sem):
    me = lax.axis_index("tp")
    k, t = ids_ref.shape
    h = t // n
    d = emb_ref.shape[2]
    vl = emb_ref.shape[0] * 8
    lo = me * vl
    loads = [pltpu.make_async_copy(du_hbm, du_s, in_sem.at[0]), pltpu.make_async_copy(w_hbm, w_s, in_sem.at[1])]
    for c in loads:
        c.start()

    def find(m, owner, cnt):
        def one(j, cnt):
            v = ids_ref[m, owner * h + j] - lo
            own = (v >= 0) & (v < vl)

            @pl.when(own)
            def _():
                pltpu.make_async_copy(emb_ref.at[v // 8], buf.at[cnt], sem).start()
                at_ref[cnt] = owner * (k * h) + m * h + j
                row_ref[cnt] = v

            return cnt + own.astype(jnp.int32)

        return lax.fori_loop(0, h, one, cnt, unroll=8)

    cnt = jnp.int32(0)
    for m in range(k):
        cnt = lax.fori_loop(0, n, functools.partial(lambda m, o, c: find(m, o, c), m), cnt)
    count_ref[0] = cnt

    pf[...] = jnp.zeros_like(pf)
    for c in loads:
        c.wait()
    cw = 512
    for m in range(k):
        def cols(i, _):
            c0 = pl.multiple_of(i * cw, cw)
            v = lax.dot_general(du_s[m], w_s[pl.ds(c0, cw), :], (((1,), (1,)), ((), ())), preferred_element_type=F32)
            d_ref[:, m * h:(m + 1) * h, pl.ds(c0, cw)] = v.astype(BF16).reshape(n, h, cw)
            return 0

        lax.fori_loop(0, d // cw, cols, 0)

    sub = lax.broadcasted_iota(jnp.int32, (8, d), 0)

    def wait(i, _):
        pltpu.make_async_copy(emb_ref.at[0], buf.at[0], sem).wait()
        return 0

    lax.fori_loop(0, cnt, wait, 0)

    def place(i, _):
        x8 = buf[i].astype(F32)
        pf[pl.ds(at_ref[i], 1)] = jnp.sum(jnp.where(sub == row_ref[i] % 8, x8, 0.0), axis=0, keepdims=True)
        return 0

    lax.fori_loop(0, cnt, place, 0)

    def pack(i, _):
        r0 = pl.multiple_of(i * ROWS, ROWS)
        p_ref[pl.ds(r0, ROWS)] = pf[pl.ds(r0, ROWS)].astype(BF16)
        return 0

    lax.fori_loop(0, (k * t) // ROWS, pack, 0)


def exchange(n, p_ref, d_ref, g_ref, dres_ref, y_ref, dg_ref,
             prx, prd, sx, sd, rx, rd, nh_s, rs_s, dgs,
             pxs, pxr, pds, pdr, xs_sem, xr_sem, ds_sem, dr_sem, gs_sem, gr_sem):
    me = lax.axis_index("tp")
    chips = n // 2
    chip, core = me // 2, me % 2
    partner = chip * 2 + 1 - core
    right = ((chip + 1) % chips) * 2 + core
    left = ((chip + chips - 1) % chips) * 2 + core
    k, h, d = dres_ref.shape

    def dev(j, same):
        return ((chip + j) % chips) * 2 + (core if same else 1 - core)

    barrier = pltpu.get_barrier_semaphore()
    for o in range(1, n):
        pl.semaphore_signal(barrier, inc=1, device_id={"tp": (me + o) % n}, device_id_type=MESH)
    pl.semaphore_wait(barrier, n - 1)

    copies = []

    def send(src, dst, ss, rs, to):
        c = pltpu.make_async_remote_copy(src_ref=src, dst_ref=dst, send_sem=ss, recv_sem=rs,
                                         device_id={"tp": to}, device_id_type=MESH)
        c.start()
        copies.append(c)

    def arrived(dst, ss, rs):
        pltpu.make_async_remote_copy(src_ref=dst, dst_ref=dst, send_sem=ss, recv_sem=rs,
                                     device_id={"tp": partner}, device_id_type=MESH).wait_recv()

    def pair_x(j):
        send(p_ref.at[dev(j, False)], prx.at[j], pxs.at[j], pxr.at[j], partner)

    def pair_d(j):
        send(d_ref.at[dev(j, False)], prd.at[j], pds.at[j], pdr.at[j], partner)

    for f, j in ((pair_x, 2), (pair_d, 2), (pair_x, 1), (pair_x, 3), (pair_d, 1), (pair_d, 3), (pair_x, 0), (pair_d, 0)):
        f(j)

    def ring(r, ss, rs, direction, chunk, src):
        send(src, r.at[direction, chunk], ss.at[direction, chunk], rs.at[direction, chunk],
             right if direction == 0 else left)

    def half(ref, j, m):
        return ref.at[j, pl.ds(m * h, h)]

    def first_hops(j, s, r, ss, rs):
        if j == 2:
            ring(r, ss, rs, 0, 0, half(s, 2, 0))
            ring(r, ss, rs, 1, 0, half(s, 2, 1))
        if j == 1:
            ring(r, ss, rs, 0, 1, half(s, 1, 1))
        if j == 3:
            ring(r, ss, rs, 1, 1, half(s, 3, 0))

    def sum_x(j):
        arrived(prx.at[j], pxs.at[j], pxr.at[j])
        sx[j] = p_ref[dev(j, True)] + prx[j]
        first_hops(j, sx, rx, xs_sem, xr_sem)

    def sum_d(j):
        arrived(prd.at[j], pds.at[j], pdr.at[j])
        sd[j] = d_ref[dev(j, True)].astype(F32) + prd[j].astype(F32)
        first_hops(j, sd, rd, ds_sem, dr_sem)

    for f, j in ((sum_x, 2), (sum_d, 2), (sum_x, 1), (sum_x, 3), (sum_d, 1), (sum_d, 3), (sum_x, 0), (sum_d, 0)):
        f(j)

    arrived(rx.at[0, 0], xs_sem.at[0, 0], xr_sem.at[0, 0])
    sx[1, :h] = sx[1, :h] + rx[0, 0]
    ring(rx, xs_sem, xr_sem, 0, 2, half(sx, 1, 0))
    arrived(rx.at[1, 0], xs_sem.at[1, 0], xr_sem.at[1, 0])
    sx[3, h:] = sx[3, h:] + rx[1, 0]
    ring(rx, xs_sem, xr_sem, 1, 2, half(sx, 3, 1))

    pieces = h // ROWS
    last = (rd.at[0, 2], rd.at[1, 2])
    for dr, j, m in ((0, 1, 0), (1, 3, 1)):
        arrived(rd.at[dr, 0], ds_sem.at[dr, 0], dr_sem.at[dr, 0])
        sd[j, m * h:(m + 1) * h] = sd[j, m * h:(m + 1) * h] + rd[dr, 0]
        for i in range(pieces):
            rows = pl.ds(i * ROWS, ROWS)
            send(sd.at[j, pl.ds(m * h + i * ROWS, ROWS)], last[dr].at[rows], ds_sem.at[dr, 2 + i],
                 dr_sem.at[dr, 2 + i], right if dr == 0 else left)

    for dr, c in ((0, 1), (1, 1), (0, 2), (1, 2)):
        arrived(rx.at[dr, c], xs_sem.at[dr, c], xr_sem.at[dr, c])
    for m in range(k):
        ca, cb = (2, 1) if m == 0 else (1, 2)
        for i in range(pieces):
            rows = pl.ds(i * ROWS, ROWS)
            x = sx[0, pl.ds(m * h + i * ROWS, ROWS)] + rx[0, ca, rows] + rx[1, cb, rows]
            y_ref[0, m, rows] = x
            xf = x.astype(F32)
            rs = lax.rsqrt(jnp.mean(xf * xf, axis=-1, keepdims=True) + EPS)
            nh_s[m, rows] = xf * rs
            rs_s[m, rows] = jnp.broadcast_to(rs, (ROWS, rs_s.shape[-1]))

    gf = g_ref[...].astype(F32)
    dg = jnp.zeros((1, d), F32)

    def grad(m, i):
        rows = pl.ds(i * ROWS, ROWS)
        nh = nh_s[m, rows]
        gdn = gf * sd[0, pl.ds(m * h + i * ROWS, ROWS)]
        dxn = rs_s[m, rows, :1] * (gdn - nh * jnp.mean(nh * gdn, axis=-1, keepdims=True))
        y_ref[1, m, rows] = (dres_ref[m, rows].astype(F32) + dxn).astype(BF16)

    for dr in range(2):
        arrived(rd.at[dr, 1], ds_sem.at[dr, 1], dr_sem.at[dr, 1])
    for i in range(pieces):
        rows = pl.ds(i * ROWS, ROWS)
        for dr in range(2):
            arrived(last[dr].at[rows], ds_sem.at[dr, 2 + i], dr_sem.at[dr, 2 + i])
        for m in range(k):
            ca, cb = (2, 1) if m == 0 else (1, 2)
            dn = sd[0, pl.ds(m * h + i * ROWS, ROWS)] + rd[0, ca, rows] + rd[1, cb, rows]
            sd[0, pl.ds(m * h + i * ROWS, ROWS)] = dn
            dg = dg + jnp.sum(dn * nh_s[m, rows], axis=0, keepdims=True)
        if i == pieces - 1:
            dgs[me] = dg
            for o in range(1, n):
                send(dgs.at[me], dgs.at[me], gs_sem.at[o], gr_sem.at[me], (me + o) % n)
        for m in range(k):
            grad(m, i)

    for o in range(1, n):
        src = (me + o) % n
        arrived(dgs.at[src], gs_sem.at[o], gr_sem.at[src])
    total_dg = dgs[0]
    for i in range(1, n):
        total_dg = total_dg + dgs[i]
    dg_ref[...] = total_dg
    for c in copies:
        c.wait_send()


def zeros(z, de_ref, first, rows, sem):
    zr = z.shape[0]
    z[...] = jnp.zeros_like(z)
    cs = [pltpu.make_async_copy(z, de_ref.at[pl.ds(first // 8 + i * zr, zr)], sem)
          for i in range(rows // (8 * zr))]
    for c in cs:
        c.start()
    return cs


def clear_and_list(rows, y_ref, row_ref, count_ref, de_ref, x_ref, slot_ref, block_ref, blocks_ref, z, table, sem, x_sem):
    cs = zeros(z, de_ref, 0, rows, sem)
    out = pltpu.make_async_copy(y_ref.at[0], x_ref, x_sem)
    out.start()

    def reset(i, _):
        table[i] = -1
        return 0

    lax.fori_loop(0, table.shape[0], reset, 0, unroll=8)
    base = lax.axis_index("tp") * 0

    def one(i, used):
        b = row_ref[i] // 8
        s = table[b]
        fresh = s < 0
        s = jnp.where(fresh, used, s)
        table[b] = s
        block_ref[s] = b
        slot_ref[i] = s * 2 + fresh.astype(jnp.int32)
        return used + fresh.astype(jnp.int32)

    blocks_ref[0] = lax.fori_loop(0, count_ref[0], one, base)
    out.wait()
    for c in cs:
        c.wait()


def clear_rest(first, rows, y_ref, dg_ref, de_in, de_ref, z, sem):
    del y_ref, dg_ref, de_in
    for c in zeros(z, de_ref, first, rows, sem):
        c.wait()


def finish(n, at_ref, row_ref, slot_ref, block_ref, count_ref, blocks_ref, y0, yl, yr, xo, do, p0, pl_, pr, pxo, pdo,
           w_ref, du_ref, g_ref, de_in, u_ref, dw_ref, de_ref, n_s, dxf, acc, sem):
    del de_in
    me = lax.axis_index("tp")
    chips = n // 2
    chip, core = me // 2, me % 2
    k, h, d = xo.shape
    t = h * n
    gf = g_ref[...].astype(F32)
    pieces = []
    for c, parts in ((core, ((y0.at[0], y0.at[1]), (yl.at[0], yl.at[1]), (yr.at[0], yr.at[1]), (xo, do))),
                     (1 - core, ((p0.at[0], p0.at[1]), (pl_.at[0], pl_.at[1]), (pr.at[0], pr.at[1]), (pxo, pdo)))):
        for off, (x, dx) in zip((0, chips - 1, 1, 2), parts):
            pieces.append((((chip + off) % chips) * 2 + c, x, dx))

    for owner, _, dx in pieces:
        for m in range(k):
            for s in range(h // ROWS):
                dxf[pl.ds(pl.multiple_of(owner * (k * h) + m * h + s * ROWS, ROWS), ROWS)] = dx[m, pl.ds(s * ROWS, ROWS)].astype(F32)

    sub = lax.broadcasted_iota(jnp.int32, (8, d), 0)
    cnt, used = count_ref[0], blocks_ref[0]

    def drain(i, _):
        pltpu.make_async_copy(acc.at[0], de_ref.at[0], sem).wait()
        return 0

    def turn(q, _):
        @pl.when(q > 0)
        def _():
            lax.fori_loop(0, SLOTS, drain, 0)

        def one(i, _):
            code = slot_ref[i]
            s = code // 2 - q * SLOTS

            @pl.when((s >= 0) & (s < SLOTS))
            def _():
                row = jnp.where(sub == row_ref[i] % 8, jnp.broadcast_to(dxf[pl.ds(at_ref[i], 1)], (8, d)), 0.0)
                acc[s] = row + jnp.where(code % 2 == 1, jnp.zeros((8, d), F32), acc[s])

            return 0

        lax.fori_loop(0, cnt, one, 0)

        def put(i, _):
            pltpu.make_async_copy(acc.at[i], de_ref.at[block_ref[q * SLOTS + i]], sem).start()
            return 0

        lax.fori_loop(0, jnp.minimum(used - q * SLOTS, SLOTS), put, 0)
        return 0

    turns = (used + SLOTS - 1) // SLOTS
    lax.fori_loop(0, turns, turn, 0)

    for owner, x, _ in pieces:
        for m in range(k):
            for s in range(h // ROWS):
                xf = x[m, pl.ds(s * ROWS, ROWS)].astype(F32)
                rs = lax.rsqrt(jnp.mean(xf * xf, axis=-1, keepdims=True) + EPS)
                n_s[pl.ds(pl.multiple_of(m * t + owner * h + s * ROWS, ROWS), ROWS)] = ((xf * rs) * gf).astype(BF16)

    w = w_ref[...]
    for m in range(k):
        u_ref[m] = jnp.dot(n_s[m * t:(m + 1) * t], w, preferred_element_type=F32).astype(BF16)
    cw = 512

    def wgrad(i, _):
        c0 = pl.multiple_of(i * cw, cw)
        v = jnp.zeros((cw, w_ref.shape[1]), F32)
        for m in range(k):
            v = v + lax.dot_general(n_s[m * t:(m + 1) * t, pl.ds(c0, cw)], du_ref[m], (((0,), (0,)), ((), ())),
                                    preferred_element_type=F32)
        dw_ref[pl.ds(c0, cw)] = v
        return 0

    lax.fori_loop(0, d // cw, wgrad, 0)
    lax.fori_loop(0, used - jnp.maximum(turns - 1, 0) * SLOTS, drain, 0)


def solution(mesh):
    n = mesh.shape["tp"]
    chips = n // 2
    to_right = [(r, (r + 2) % n) for r in range(n)]
    to_left = [(r, (r + n - 2) % n) for r in range(n)]
    to_partner = [(r, r ^ 1) for r in range(n)]
    dma = pltpu.SemaphoreType.DMA

    def local(ids, emb, g, w, du, dres):
        k, t = ids.shape
        vl, d = emb.shape
        f = w.shape[1]
        h = t // n
        kt = k * t
        g2 = g.reshape(1, d)
        i32 = lambda *s: jax.ShapeDtypeStruct(s, jnp.int32)
        cost = lambda b: pl.CostEstimate(flops=0, bytes_accessed=b, transcendentals=0)

        rows, part, at, row, count = pl.pallas_call(
            functools.partial(lookup, n),
            out_shape=(jax.ShapeDtypeStruct((kt, d), BF16), jax.ShapeDtypeStruct((n, k * h, d), BF16),
                       i32(kt), i32(kt), i32(1)),
            in_specs=[SMEM, ANY, ANY, ANY],
            out_specs=(VMEM, VMEM, SMEM, SMEM, SMEM),
            scratch_shapes=[
                pltpu.VMEM((k, t, f), BF16), pltpu.VMEM((d, f), BF16), pltpu.VMEM((kt, 8, d), BF16),
                pltpu.VMEM((kt, d), F32), dma, dma((2,)),
            ],
            compiler_params=pltpu.CompilerParams(vmem_limit_bytes=32 << 20),
            name="lookup",
        )(ids, emb.reshape(vl // 8, 8, d), du, w)

        y, dg = pl.pallas_call(
            functools.partial(exchange, n),
            out_shape=(jax.ShapeDtypeStruct((2, k, h, d), BF16), jax.ShapeDtypeStruct((1, d), F32)),
            in_specs=[VMEM] * 4,
            out_specs=(VMEM, VMEM),
            scratch_shapes=[
                pltpu.VMEM((chips, k * h, d), BF16),
                pltpu.VMEM((chips, k * h, d), BF16),
                pltpu.VMEM((chips, k * h, d), BF16),
                pltpu.VMEM((chips, k * h, d), F32),
                pltpu.VMEM((2, 3, h, d), BF16),
                pltpu.VMEM((2, 3, h, d), F32),
                pltpu.VMEM((k, h, d), F32),
                pltpu.VMEM((k, h, 128), F32),
                pltpu.VMEM((n, 1, d), F32),
                dma((chips,)), dma((chips,)), dma((chips,)), dma((chips,)),
                dma((2, 3)), dma((2, 3)), dma((2, 2 + h // ROWS)), dma((2, 2 + h // ROWS)),
                dma((n,)), dma((n,)),
            ],
            compiler_params=pltpu.CompilerParams(collective_id=0, has_side_effects=True, vmem_limit_bytes=24 << 20),
            name="exchange",
        )(rows.reshape(n, k * h, d), part, g2, dres)

        yl = lax.ppermute(y, "tp", to_right)
        yr = lax.ppermute(y, "tp", to_left)
        py = lax.ppermute(y, "tp", to_partner)
        xo = lax.ppermute(yl[0], "tp", to_right)
        do = lax.ppermute(yr[1], "tp", to_left)
        pyl = lax.ppermute(yl, "tp", to_partner)
        pyr = lax.ppermute(yr, "tp", to_partner)
        pxo = lax.ppermute(xo, "tp", to_partner)
        pdo = lax.ppermute(do, "tp", to_partner)

        zr = 512
        split = (vl * 5 // 8) // zr * zr
        de_shape = jax.ShapeDtypeStruct((vl // 8, 8, d), F32)
        de, x, slot, block, blocks = pl.pallas_call(
            functools.partial(clear_and_list, split),
            out_shape=(de_shape, jax.ShapeDtypeStruct((k, h, d), BF16), i32(kt), i32(kt), i32(1)),
            in_specs=[VMEM, SMEM, SMEM],
            out_specs=(ANY, ANY, SMEM, SMEM, SMEM),
            scratch_shapes=[pltpu.VMEM((zr // 8, 8, d), F32), pltpu.SMEM((vl // 8,), jnp.int32), dma, dma],
            compiler_params=pltpu.CompilerParams(vmem_limit_bytes=8 << 20),
            cost_estimate=cost(split * d * 4),
            name="clear0",
        )(y, row, count)
        dgf = dg.reshape(d)
        de = pl.pallas_call(
            functools.partial(clear_rest, split, vl - split),
            out_shape=de_shape,
            in_specs=[ANY, ANY, ANY], out_specs=ANY,
            input_output_aliases={2: 0},
            scratch_shapes=[pltpu.VMEM((zr // 8, 8, d), F32), dma],
            compiler_params=pltpu.CompilerParams(vmem_limit_bytes=8 << 20),
            cost_estimate=cost((vl - split) * d * 4),
            name="clear1",
        )(yl, dgf, de)

        u, dw, de = pl.pallas_call(
            functools.partial(finish, n),
            out_shape=(jax.ShapeDtypeStruct((k, t, f), BF16), jax.ShapeDtypeStruct((d, f), F32), de_shape),
            in_specs=[SMEM] * 6 + [VMEM] * 13 + [ANY],
            out_specs=(VMEM, VMEM, ANY),
            input_output_aliases={19: 2},
            scratch_shapes=[
                pltpu.VMEM((kt, d), BF16),
                pltpu.VMEM((kt, d), F32),
                pltpu.VMEM((SLOTS, 8, d), F32),
                dma,
            ],
            compiler_params=pltpu.CompilerParams(vmem_limit_bytes=36 << 20),
            name="finish",
        )(at, row, slot, block, count, blocks, y, yl, yr, xo, do, py, pyl, pyr, pxo, pdo, w, du, g2, de)
        return u, x, de.reshape(vl, d), dw, dgf

    return jax.shard_map(
        local,
        mesh=mesh,
        in_specs=(P("dp", None), P("tp", None), P(None), P(None, "tp"), P("dp", None, "tp"), P("dp", "tp", None)),
        out_specs=(P("dp", None, "tp"), P("dp", "tp", None), P(("dp", "tp"), None), P(None, ("dp", "tp")), P("dp")),
        check_vma=False,
    )
```

```python
import functools

import jax
import jax.numpy as jnp
from jax import lax
from jax.experimental import pallas as pl
from jax.experimental.pallas import tpu as pltpu
from jax.sharding import PartitionSpec as P


EPS = 1e-6
MESH = pl.DeviceIdType.MESH
VMEM = pl.BlockSpec(memory_space=pltpu.VMEM)
SMEM = pl.BlockSpec(memory_space=pltpu.SMEM)
ANY = pl.BlockSpec(memory_space=pl.ANY)
HBM = pl.BlockSpec(memory_space=pltpu.HBM)
F32 = jnp.float32
BF16 = jnp.bfloat16
ROWS = 16
SLOTS = 128


def lookup(n, ids_ref, emb_ref, p_ref, at_ref, row_ref, count_ref, buf, pf, found, sem):
    me = lax.axis_index("tp")
    k, t = ids_ref.shape
    h = t // n
    d = emb_ref.shape[2]
    vl = emb_ref.shape[0] * 8
    lo = me * vl

    cnt = jnp.int32(0)
    for m in range(k):
        def find(i, cnt):
            v = ids_ref[m, i]
            found[cnt] = i
            return cnt + ((v >= lo) & (v < lo + vl)).astype(jnp.int32)

        first = cnt
        cnt = lax.fori_loop(0, t, find, first, unroll=16)

        def fetch(c, _):
            i = found[c]
            v = ids_ref[m, i] - lo
            pltpu.make_async_copy(emb_ref.at[v // 8], buf.at[c], sem).start()
            at_ref[c] = (i // h) * (k * h) + m * h + i % h
            row_ref[c] = v
            return 0

        lax.fori_loop(first, cnt, fetch, 0)
    count_ref[0] = cnt

    pf[...] = jnp.zeros_like(pf)
    sub = lax.broadcasted_iota(jnp.int32, (8, d), 0)

    def wait(i, _):
        pltpu.make_async_copy(emb_ref.at[0], buf.at[0], sem).wait()
        return 0

    lax.fori_loop(0, cnt, wait, 0)
    step = 4

    def place(q, _):
        rows = []
        for u in range(step):
            i = jnp.minimum(q * step + u, cnt - 1)
            x8 = buf[i].astype(F32)
            rows.append((at_ref[i], jnp.sum(jnp.where(sub == row_ref[i] % 8, x8, 0.0), axis=0, keepdims=True)))
        for at, x in rows:
            pf[pl.ds(at, 1)] = x
        return 0

    lax.fori_loop(0, (cnt + step - 1) // step, place, 0)

    def pack(i, _):
        r0 = pl.multiple_of(i * ROWS, ROWS)
        p_ref[pl.ds(r0, ROWS)] = pf[pl.ds(r0, ROWS)].astype(BF16)
        return 0

    lax.fori_loop(0, (k * t) // ROWS, pack, 0)


def exchange(n, p_ref, du_ref, w_ref, g_ref, dres_ref, y_ref, dg_ref,
             d_ref, prx, prd, sx, sd, rx, rd, nh_s, rs_s, dgs,
             pxs, pxr, pds, pdr, xs_sem, xr_sem, ds_sem, dr_sem, gs_sem, gr_sem):
    me = lax.axis_index("tp")
    chips = n // 2
    chip, core = me // 2, me % 2
    partner = chip * 2 + 1 - core
    right = ((chip + 1) % chips) * 2 + core
    left = ((chip + chips - 1) % chips) * 2 + core
    k, h, d = dres_ref.shape

    def dev(j, same):
        return ((chip + j) % chips) * 2 + (core if same else 1 - core)

    barrier = pltpu.get_barrier_semaphore()
    for o in range(1, n):
        pl.semaphore_signal(barrier, inc=1, device_id={"tp": (me + o) % n}, device_id_type=MESH)
    pl.semaphore_wait(barrier, n - 1)

    copies = []

    def send(src, dst, ss, rs, to):
        c = pltpu.make_async_remote_copy(src_ref=src, dst_ref=dst, send_sem=ss, recv_sem=rs,
                                         device_id={"tp": to}, device_id_type=MESH)
        c.start()
        copies.append(c)

    def arrived(dst, ss, rs):
        pltpu.make_async_remote_copy(src_ref=dst, dst_ref=dst, send_sem=ss, recv_sem=rs,
                                     device_id={"tp": partner}, device_id_type=MESH).wait_recv()

    def pair_x(j):
        send(p_ref.at[dev(j, False)], prx.at[j], pxs.at[j], pxr.at[j], partner)

    def pair_d(j):
        send(d_ref.at[dev(j, False)], prd.at[j], pds.at[j], pdr.at[j], partner)

    for j in (2, 1, 3, 0):
        pair_x(j)

    def ring(r, ss, rs, direction, chunk, src):
        send(src, r.at[direction, chunk], ss.at[direction, chunk], rs.at[direction, chunk],
             right if direction == 0 else left)

    def half(ref, j, m):
        return ref.at[j, pl.ds(m * h, h)]

    def first_hops(j, s, r, ss, rs):
        if j == 2:
            ring(r, ss, rs, 0, 0, half(s, 2, 0))
            ring(r, ss, rs, 1, 0, half(s, 2, 1))
        if j == 1:
            ring(r, ss, rs, 0, 1, half(s, 1, 1))
        if j == 3:
            ring(r, ss, rs, 1, 1, half(s, 3, 0))

    def sum_x(j):
        arrived(prx.at[j], pxs.at[j], pxr.at[j])
        sx[j] = p_ref[dev(j, True)] + prx[j]
        first_hops(j, sx, rx, xs_sem, xr_sem)

    def sum_d(j):
        arrived(prd.at[j], pds.at[j], pdr.at[j])
        sd[j] = d_ref[dev(j, True)].astype(F32) + prd[j].astype(F32)
        first_hops(j, sd, rd, ds_sem, dr_sem)

    for j in (2, 1, 3):
        sum_x(j)
    cw = 512
    for m in range(k):
        def cols(i, _):
            c0 = pl.multiple_of(i * cw, cw)
            v = lax.dot_general(du_ref[m], w_ref[pl.ds(c0, cw), :], (((1,), (1,)), ((), ())), preferred_element_type=F32)
            d_ref[:, m * h:(m + 1) * h, pl.ds(c0, cw)] = v.astype(BF16).reshape(n, h, cw)
            return 0

        lax.fori_loop(0, d // cw, cols, 0)
    for j in (2, 1, 3, 0):
        pair_d(j)
    for j in (2, 1, 3, 0):
        sum_d(j)
    sum_x(0)

    arrived(rx.at[0, 0], xs_sem.at[0, 0], xr_sem.at[0, 0])
    sx[1, :h] = sx[1, :h] + rx[0, 0]
    ring(rx, xs_sem, xr_sem, 0, 2, half(sx, 1, 0))
    arrived(rx.at[1, 0], xs_sem.at[1, 0], xr_sem.at[1, 0])
    sx[3, h:] = sx[3, h:] + rx[1, 0]
    ring(rx, xs_sem, xr_sem, 1, 2, half(sx, 3, 1))

    pieces = h // ROWS
    last = (rd.at[0, 2], rd.at[1, 2])
    for dr, j, m in ((0, 1, 0), (1, 3, 1)):
        arrived(rd.at[dr, 0], ds_sem.at[dr, 0], dr_sem.at[dr, 0])
        sd[j, m * h:(m + 1) * h] = sd[j, m * h:(m + 1) * h] + rd[dr, 0]
        for i in range(pieces):
            rows = pl.ds(i * ROWS, ROWS)
            send(sd.at[j, pl.ds(m * h + i * ROWS, ROWS)], last[dr].at[rows], ds_sem.at[dr, 2 + i],
                 dr_sem.at[dr, 2 + i], right if dr == 0 else left)

    for dr, c in ((0, 1), (1, 1), (0, 2), (1, 2)):
        arrived(rx.at[dr, c], xs_sem.at[dr, c], xr_sem.at[dr, c])
    for m in range(k):
        ca, cb = (2, 1) if m == 0 else (1, 2)
        for i in range(pieces):
            rows = pl.ds(i * ROWS, ROWS)
            x = sx[0, pl.ds(m * h + i * ROWS, ROWS)] + rx[0, ca, rows] + rx[1, cb, rows]
            y_ref[0, m, rows] = x
            xf = x.astype(F32)
            rs = lax.rsqrt(jnp.mean(xf * xf, axis=-1, keepdims=True) + EPS)
            nh_s[m, rows] = xf * rs
            rs_s[m, rows] = jnp.broadcast_to(rs, (ROWS, rs_s.shape[-1]))

    gf = g_ref[...].astype(F32).reshape(1, d)
    dg = jnp.zeros((1, d), F32)

    def grad(m, i):
        rows = pl.ds(i * ROWS, ROWS)
        nh = nh_s[m, rows]
        gdn = gf * sd[0, pl.ds(m * h + i * ROWS, ROWS)]
        dxn = rs_s[m, rows, :1] * (gdn - nh * jnp.mean(nh * gdn, axis=-1, keepdims=True))
        y_ref[1, m, rows] = (dres_ref[m, rows].astype(F32) + dxn).astype(BF16)

    for dr in range(2):
        arrived(rd.at[dr, 1], ds_sem.at[dr, 1], dr_sem.at[dr, 1])
    for i in range(pieces):
        rows = pl.ds(i * ROWS, ROWS)
        for dr in range(2):
            arrived(last[dr].at[rows], ds_sem.at[dr, 2 + i], dr_sem.at[dr, 2 + i])
        for m in range(k):
            ca, cb = (2, 1) if m == 0 else (1, 2)
            dn = sd[0, pl.ds(m * h + i * ROWS, ROWS)] + rd[0, ca, rows] + rd[1, cb, rows]
            sd[0, pl.ds(m * h + i * ROWS, ROWS)] = dn
            dg = dg + jnp.sum(dn * nh_s[m, rows], axis=0, keepdims=True)
        if i == pieces - 1:
            dgs[me] = dg
            for o in range(1, n):
                send(dgs.at[me], dgs.at[me], gs_sem.at[o], gr_sem.at[me], (me + o) % n)
        for m in range(k):
            grad(m, i)

    for o in range(1, n):
        src = (me + o) % n
        arrived(dgs.at[src], gs_sem.at[o], gr_sem.at[src])
    total_dg = dgs[0]
    for i in range(1, n):
        total_dg = total_dg + dgs[i]
    dg_ref[...] = total_dg
    for c in copies:
        c.wait_send()


def zeros(z, de_ref, first, rows, sem):
    zr = z.shape[0]
    z[...] = jnp.zeros_like(z)
    cs = [pltpu.make_async_copy(z, de_ref.at[pl.ds(first // 8 + i * zr, zr)], sem)
          for i in range(rows // (8 * zr))]
    for c in cs:
        c.start()
    return cs


def clear_and_list(rows, y_ref, row_ref, count_ref, de_ref, x_ref, slot_ref, block_ref, blocks_ref, z, table, sem, x_sem):
    cs = zeros(z, de_ref, 0, rows, sem)
    out = pltpu.make_async_copy(y_ref.at[0], x_ref, x_sem)
    out.start()

    def reset(i, _):
        table[i] = -1
        return 0

    lax.fori_loop(0, table.shape[0], reset, 0, unroll=8)
    base = lax.axis_index("tp") * 0

    def one(i, used):
        b = row_ref[i] // 8
        s = table[b]
        fresh = s < 0
        s = jnp.where(fresh, used, s)
        table[b] = s
        block_ref[s] = b
        slot_ref[i] = s * 2 + fresh.astype(jnp.int32)
        return used + fresh.astype(jnp.int32)

    blocks_ref[0] = lax.fori_loop(0, count_ref[0], one, base)
    out.wait()
    for c in cs:
        c.wait()


def clear_rest(first, rows, y_ref, dg_in, de_in, de_ref, dg_ref, z, sem):
    del y_ref, de_in
    dg_ref[...] = dg_in[...].reshape(dg_ref.shape)
    for c in zeros(z, de_ref, first, rows, sem):
        c.wait()


def finish(n, at_ref, row_ref, slot_ref, block_ref, count_ref, blocks_ref, y0, yl, yr, xo, do, p0, pl_, pr, pxo, pdo,
           w_ref, du_ref, g_ref, de_in, u_ref, dw_ref, de_ref, n_s, dxf, acc, sem):
    del de_in
    me = lax.axis_index("tp")
    chips = n // 2
    chip, core = me // 2, me % 2
    k, h, d = xo.shape
    t = h * n
    gf = g_ref[...].astype(F32).reshape(1, d)
    pieces = []
    for c, parts in ((core, ((y0.at[0], y0.at[1]), (yl.at[0], yl.at[1]), (yr.at[0], yr.at[1]), (xo, do))),
                     (1 - core, ((p0.at[0], p0.at[1]), (pl_.at[0], pl_.at[1]), (pr.at[0], pr.at[1]), (pxo, pdo)))):
        for off, (x, dx) in zip((0, chips - 1, 1, 2), parts):
            pieces.append((((chip + off) % chips) * 2 + c, x, dx))

    for owner, _, dx in pieces:
        for m in range(k):
            for s in range(h // ROWS):
                dxf[pl.ds(pl.multiple_of(owner * (k * h) + m * h + s * ROWS, ROWS), ROWS)] = dx[m, pl.ds(s * ROWS, ROWS)].astype(F32)

    sub = lax.broadcasted_iota(jnp.int32, (8, d), 0)
    cnt, used = count_ref[0], blocks_ref[0]

    def drain(i, _):
        pltpu.make_async_copy(acc.at[0], de_ref.at[0], sem).wait()
        return 0

    def turn(q, _):
        @pl.when(q > 0)
        def _():
            lax.fori_loop(0, SLOTS, drain, 0)

        def one(i, _):
            code = slot_ref[i]
            s = code // 2 - q * SLOTS

            @pl.when((s >= 0) & (s < SLOTS))
            def _():
                row = jnp.where(sub == row_ref[i] % 8, jnp.broadcast_to(dxf[pl.ds(at_ref[i], 1)], (8, d)), 0.0)
                acc[s] = row + jnp.where(code % 2 == 1, jnp.zeros((8, d), F32), acc[s])

            return 0

        lax.fori_loop(0, cnt, one, 0)

        def put(i, _):
            pltpu.make_async_copy(acc.at[i], de_ref.at[block_ref[q * SLOTS + i]], sem).start()
            return 0

        lax.fori_loop(0, jnp.minimum(used - q * SLOTS, SLOTS), put, 0)
        return 0

    turns = (used + SLOTS - 1) // SLOTS
    lax.fori_loop(0, turns, turn, 0)

    for owner, x, _ in pieces:
        for m in range(k):
            for s in range(h // ROWS):
                xf = x[m, pl.ds(s * ROWS, ROWS)].astype(F32)
                rs = lax.rsqrt(jnp.mean(xf * xf, axis=-1, keepdims=True) + EPS)
                n_s[pl.ds(pl.multiple_of(m * t + owner * h + s * ROWS, ROWS), ROWS)] = ((xf * rs) * gf).astype(BF16)

    w = w_ref[...]
    for m in range(k):
        u_ref[m] = jnp.dot(n_s[m * t:(m + 1) * t], w, preferred_element_type=F32).astype(BF16)
    cw = 512

    def wgrad(i, _):
        c0 = pl.multiple_of(i * cw, cw)
        v = jnp.zeros((cw, w_ref.shape[1]), F32)
        for m in range(k):
            v = v + lax.dot_general(n_s[m * t:(m + 1) * t, pl.ds(c0, cw)], du_ref[m], (((0,), (0,)), ((), ())),
                                    preferred_element_type=F32)
        dw_ref[pl.ds(c0, cw)] = v
        return 0

    lax.fori_loop(0, d // cw, wgrad, 0)
    lax.fori_loop(0, used - jnp.maximum(turns - 1, 0) * SLOTS, drain, 0)


def solution(mesh):
    n = mesh.shape["tp"]
    chips = n // 2
    to_right = [(r, (r + 2) % n) for r in range(n)]
    to_left = [(r, (r + n - 2) % n) for r in range(n)]
    to_partner = [(r, r ^ 1) for r in range(n)]
    dma = pltpu.SemaphoreType.DMA

    def step(ids, emb, g, w, du, dres):
        k, t = ids.shape
        vl, d = emb.shape
        f = w.shape[1]
        h = t // n
        kt = k * t
        i32 = lambda *s: jax.ShapeDtypeStruct(s, jnp.int32)
        cost = lambda b: pl.CostEstimate(flops=0, bytes_accessed=b, transcendentals=0)

        rows, at, row, count = pl.pallas_call(
            functools.partial(lookup, n),
            out_shape=(jax.ShapeDtypeStruct((kt, d), BF16), i32(kt), i32(kt), i32(1)),
            in_specs=[SMEM, HBM],
            out_specs=(VMEM, SMEM, SMEM, SMEM),
            scratch_shapes=[
                pltpu.VMEM((kt, 8, d), BF16), pltpu.VMEM((kt, d), F32), pltpu.SMEM((kt + 1,), jnp.int32), dma,
            ],
            compiler_params=pltpu.CompilerParams(vmem_limit_bytes=32 << 20),
            cost_estimate=cost(4 << 20),
            name="lookup",
        )(ids, emb.reshape(vl // 8, 8, d))

        y, dg = pl.pallas_call(
            functools.partial(exchange, n),
            out_shape=(jax.ShapeDtypeStruct((2, k, h, d), BF16), jax.ShapeDtypeStruct((1, d), F32)),
            in_specs=[VMEM] * 5,
            out_specs=(VMEM, VMEM),
            scratch_shapes=[
                pltpu.VMEM((n, k * h, d), BF16),
                pltpu.VMEM((chips, k * h, d), BF16),
                pltpu.VMEM((chips, k * h, d), BF16),
                pltpu.VMEM((chips, k * h, d), BF16),
                pltpu.VMEM((chips, k * h, d), F32),
                pltpu.VMEM((2, 3, h, d), BF16),
                pltpu.VMEM((2, 3, h, d), F32),
                pltpu.VMEM((k, h, d), F32),
                pltpu.VMEM((k, h, 128), F32),
                pltpu.VMEM((n, 1, d), F32),
                dma((chips,)), dma((chips,)), dma((chips,)), dma((chips,)),
                dma((2, 3)), dma((2, 3)), dma((2, 2 + h // ROWS)), dma((2, 2 + h // ROWS)),
                dma((n,)), dma((n,)),
            ],
            compiler_params=pltpu.CompilerParams(collective_id=0, has_side_effects=True, vmem_limit_bytes=28 << 20),
            name="exchange",
        )(rows.reshape(n, k * h, d), du, w, g, dres)

        def move(v, perm):
            return lax.ppermute(v, "tp", perm)

        yl = move(y, to_right)
        yr = move(y, to_left)
        py = move(y, to_partner)
        xo = move(yl[0], to_right)
        do = move(yr[1], to_left)
        pyl = move(yl, to_partner)
        pyr = move(yr, to_partner)
        pxo = move(xo, to_partner)
        pdo = move(do, to_partner)

        zr = 512
        split = (vl * 5 // 8) // zr * zr
        de_shape = jax.ShapeDtypeStruct((vl // 8, 8, d), F32)
        de, x, slot, block, blocks = pl.pallas_call(
            functools.partial(clear_and_list, split),
            out_shape=(de_shape, jax.ShapeDtypeStruct((k, h, d), BF16), i32(kt), i32(kt), i32(1)),
            in_specs=[VMEM, SMEM, SMEM],
            out_specs=(ANY, ANY, SMEM, SMEM, SMEM),
            scratch_shapes=[pltpu.VMEM((zr // 8, 8, d), F32), pltpu.SMEM((vl // 8,), jnp.int32), dma, dma],
            compiler_params=pltpu.CompilerParams(vmem_limit_bytes=8 << 20),
            cost_estimate=cost(split * d * 4),
            name="clear0",
        )(y, row, count)
        de, dgf = pl.pallas_call(
            functools.partial(clear_rest, split, vl - split),
            out_shape=(de_shape, jax.ShapeDtypeStruct((d,), F32)),
            in_specs=[ANY, VMEM, ANY], out_specs=(ANY, VMEM),
            input_output_aliases={2: 0},
            scratch_shapes=[pltpu.VMEM((zr // 8, 8, d), F32), dma],
            compiler_params=pltpu.CompilerParams(vmem_limit_bytes=8 << 20),
            cost_estimate=cost((vl - split) * d * 4),
            name="clear1",
        )(yl, dg, de)

        u, dw, de = pl.pallas_call(
            functools.partial(finish, n),
            out_shape=(jax.ShapeDtypeStruct((k, t, f), BF16), jax.ShapeDtypeStruct((d, f), F32), de_shape),
            in_specs=[SMEM] * 6 + [VMEM] * 13 + [ANY],
            out_specs=(VMEM, VMEM, ANY),
            input_output_aliases={19: 2},
            scratch_shapes=[
                pltpu.VMEM((kt, d), BF16),
                pltpu.VMEM((kt, d), F32),
                pltpu.VMEM((SLOTS, 8, d), F32),
                dma,
            ],
            compiler_params=pltpu.CompilerParams(vmem_limit_bytes=36 << 20),
            name="finish",
        )(at, row, slot, block, count, blocks, y, yl, yr, xo, do, py, pyl, pyr, pxo, pdo, w, du, g, de)
        return u, x, de.reshape(vl, d), dw, dgf

    return jax.shard_map(
        step,
        mesh=mesh,
        in_specs=(P("dp", None), P("tp", None), P(None), P(None, "tp"), P("dp", None, "tp"), P("dp", "tp", None)),
        out_specs=(P("dp", None, "tp"), P("dp", "tp", None), P(("dp", "tp"), None), P(None, ("dp", "tp")), P("dp")),
        check_vma=False,
    )
```

```python
import functools

import jax
import jax.numpy as jnp
from jax import lax
from jax.experimental import pallas as pl
from jax.experimental.pallas import tpu as pltpu
from jax.sharding import PartitionSpec as P


EPS = 1e-6
MESH = pl.DeviceIdType.MESH
VMEM = pl.BlockSpec(memory_space=pltpu.VMEM)
SMEM = pl.BlockSpec(memory_space=pltpu.SMEM)
ANY = pl.BlockSpec(memory_space=pl.ANY)
HBM = pl.BlockSpec(memory_space=pltpu.HBM)
F32 = jnp.float32
BF16 = jnp.bfloat16
ROWS = 16
SLOTS = 128


def slab(i, m, k, h):
    return lax.div(i, h) * (k * h) + m * h + lax.rem(i, h)


def lookup(n, ids_ref, emb_ref, p_ref, buf, pf, found, at_s, row_s, sem):
    me = lax.axis_index("tp")
    k, t = ids_ref.shape
    h = t // n
    d = emb_ref.shape[2]
    vl = emb_ref.shape[0] * 8
    lo = me * vl

    cnt = jnp.int32(0)
    for m in range(k):
        def find(i, cnt):
            v = ids_ref[m, i]
            found[cnt] = i
            return cnt + ((v >= lo) & (v < lo + vl)).astype(jnp.int32)

        first = cnt
        cnt = lax.fori_loop(0, t, find, first, unroll=16)

        def fetch(c, _):
            i = found[c]
            v = ids_ref[m, i] - lo
            pltpu.make_async_copy(emb_ref.at[lax.div(v, 8)], buf.at[c], sem).start()
            at_s[c] = slab(i, m, k, h)
            row_s[c] = lax.rem(v, 8)
            return 0

        lax.fori_loop(first, cnt, fetch, 0)

    pf[...] = jnp.zeros_like(pf)
    sub = lax.broadcasted_iota(jnp.int32, (8, d), 0)

    def wait(i, _):
        pltpu.make_async_copy(emb_ref.at[0], buf.at[0], sem).wait()
        return 0

    lax.fori_loop(0, cnt, wait, 0)
    step = 4

    def place(q, _):
        rows = []
        for u in range(step):
            i = jnp.minimum(q * step + u, cnt - 1)
            x8 = buf[i].astype(F32)
            rows.append((at_s[i], jnp.sum(jnp.where(sub == row_s[i], x8, 0.0), axis=0, keepdims=True)))
        for at, x in rows:
            pf[pl.ds(at, 1)] = x
        return 0

    lax.fori_loop(0, lax.div(cnt + step - 1, step), place, 0)

    def pack(i, _):
        r0 = pl.multiple_of(i * ROWS, ROWS)
        p_ref[pl.ds(r0, ROWS)] = pf[pl.ds(r0, ROWS)].astype(BF16)
        return 0

    lax.fori_loop(0, (k * t) // ROWS, pack, 0)


def exchange(n, p_ref, du_ref, w_ref, g_ref, dres_ref, y_ref, dg_ref,
             d_ref, prx, prd, sx, sd, rx, rd, nh_s, rs_s, dgs,
             pxs, pxr, pds, pdr, xs_sem, xr_sem, ds_sem, dr_sem, gs_sem, gr_sem):
    me = lax.axis_index("tp")
    chips = n // 2
    chip, core = me // 2, me % 2
    partner = chip * 2 + 1 - core
    right = ((chip + 1) % chips) * 2 + core
    left = ((chip + chips - 1) % chips) * 2 + core
    k, h, d = dres_ref.shape

    def dev(j, same):
        return ((chip + j) % chips) * 2 + (core if same else 1 - core)

    barrier = pltpu.get_barrier_semaphore()
    for o in range(1, n):
        pl.semaphore_signal(barrier, inc=1, device_id={"tp": (me + o) % n}, device_id_type=MESH)
    pl.semaphore_wait(barrier, n - 1)

    copies = []

    def send(src, dst, ss, rs, to):
        c = pltpu.make_async_remote_copy(src_ref=src, dst_ref=dst, send_sem=ss, recv_sem=rs,
                                         device_id={"tp": to}, device_id_type=MESH)
        c.start()
        copies.append(c)

    def arrived(dst, ss, rs):
        pltpu.make_async_remote_copy(src_ref=dst, dst_ref=dst, send_sem=ss, recv_sem=rs,
                                     device_id={"tp": partner}, device_id_type=MESH).wait_recv()

    def pair_x(j):
        send(p_ref.at[dev(j, False)], prx.at[j], pxs.at[j], pxr.at[j], partner)

    def pair_d(j):
        send(d_ref.at[dev(j, False)], prd.at[j], pds.at[j], pdr.at[j], partner)

    for j in (2, 1, 3, 0):
        pair_x(j)

    def ring(r, ss, rs, direction, chunk, src):
        send(src, r.at[direction, chunk], ss.at[direction, chunk], rs.at[direction, chunk],
             right if direction == 0 else left)

    def half(ref, j, m):
        return ref.at[j, pl.ds(m * h, h)]

    def first_hops(j, s, r, ss, rs):
        if j == 2:
            ring(r, ss, rs, 0, 0, half(s, 2, 0))
            ring(r, ss, rs, 1, 0, half(s, 2, 1))
        if j == 1:
            ring(r, ss, rs, 0, 1, half(s, 1, 1))
        if j == 3:
            ring(r, ss, rs, 1, 1, half(s, 3, 0))

    def sum_x(j):
        arrived(prx.at[j], pxs.at[j], pxr.at[j])
        sx[j] = p_ref[dev(j, True)] + prx[j]
        first_hops(j, sx, rx, xs_sem, xr_sem)

    def sum_d(j):
        arrived(prd.at[j], pds.at[j], pdr.at[j])
        sd[j] = d_ref[dev(j, True)].astype(F32) + prd[j].astype(F32)
        first_hops(j, sd, rd, ds_sem, dr_sem)

    for j in (2, 1, 3):
        sum_x(j)
    cw = 512
    for m in range(k):
        def cols(i, _):
            c0 = pl.multiple_of(i * cw, cw)
            v = lax.dot_general(du_ref[m], w_ref[pl.ds(c0, cw), :], (((1,), (1,)), ((), ())), preferred_element_type=F32)
            d_ref[:, m * h:(m + 1) * h, pl.ds(c0, cw)] = v.astype(BF16).reshape(n, h, cw)
            return 0

        lax.fori_loop(0, d // cw, cols, 0)
    for j in (2, 1, 3, 0):
        pair_d(j)
    for j in (2, 1, 3, 0):
        sum_d(j)
    sum_x(0)

    arrived(rx.at[0, 0], xs_sem.at[0, 0], xr_sem.at[0, 0])
    sx[1, :h] = sx[1, :h] + rx[0, 0]
    ring(rx, xs_sem, xr_sem, 0, 2, half(sx, 1, 0))
    arrived(rx.at[1, 0], xs_sem.at[1, 0], xr_sem.at[1, 0])
    sx[3, h:] = sx[3, h:] + rx[1, 0]
    ring(rx, xs_sem, xr_sem, 1, 2, half(sx, 3, 1))

    pieces = h // ROWS
    last = (rd.at[0, 2], rd.at[1, 2])
    for dr, j, m in ((0, 1, 0), (1, 3, 1)):
        arrived(rd.at[dr, 0], ds_sem.at[dr, 0], dr_sem.at[dr, 0])
        sd[j, m * h:(m + 1) * h] = sd[j, m * h:(m + 1) * h] + rd[dr, 0]
        for i in range(pieces):
            rows = pl.ds(i * ROWS, ROWS)
            send(sd.at[j, pl.ds(m * h + i * ROWS, ROWS)], last[dr].at[rows], ds_sem.at[dr, 2 + i],
                 dr_sem.at[dr, 2 + i], right if dr == 0 else left)

    for dr, c in ((0, 1), (1, 1), (0, 2), (1, 2)):
        arrived(rx.at[dr, c], xs_sem.at[dr, c], xr_sem.at[dr, c])
    for m in range(k):
        ca, cb = (2, 1) if m == 0 else (1, 2)
        for i in range(pieces):
            rows = pl.ds(i * ROWS, ROWS)
            x = sx[0, pl.ds(m * h + i * ROWS, ROWS)] + rx[0, ca, rows] + rx[1, cb, rows]
            y_ref[0, m, rows] = x
            xf = x.astype(F32)
            rs = lax.rsqrt(jnp.mean(xf * xf, axis=-1, keepdims=True) + EPS)
            nh_s[m, rows] = xf * rs
            rs_s[m, rows] = jnp.broadcast_to(rs, (ROWS, rs_s.shape[-1]))

    gf = g_ref[...].astype(F32).reshape(1, d)
    dg = jnp.zeros((1, d), F32)

    def grad(m, i):
        rows = pl.ds(i * ROWS, ROWS)
        nh = nh_s[m, rows]
        gdn = gf * sd[0, pl.ds(m * h + i * ROWS, ROWS)]
        dxn = rs_s[m, rows, :1] * (gdn - nh * jnp.mean(nh * gdn, axis=-1, keepdims=True))
        y_ref[1, m, rows] = (dres_ref[m, rows].astype(F32) + dxn).astype(BF16)

    for dr in range(2):
        arrived(rd.at[dr, 1], ds_sem.at[dr, 1], dr_sem.at[dr, 1])
    for i in range(pieces):
        rows = pl.ds(i * ROWS, ROWS)
        for dr in range(2):
            arrived(last[dr].at[rows], ds_sem.at[dr, 2 + i], dr_sem.at[dr, 2 + i])
        for m in range(k):
            ca, cb = (2, 1) if m == 0 else (1, 2)
            dn = sd[0, pl.ds(m * h + i * ROWS, ROWS)] + rd[0, ca, rows] + rd[1, cb, rows]
            sd[0, pl.ds(m * h + i * ROWS, ROWS)] = dn
            dg = dg + jnp.sum(dn * nh_s[m, rows], axis=0, keepdims=True)
        if i == pieces - 1:
            dgs[me] = dg
            for o in range(1, n):
                send(dgs.at[me], dgs.at[me], gs_sem.at[o], gr_sem.at[me], (me + o) % n)
        for m in range(k):
            grad(m, i)

    for o in range(1, n):
        src = (me + o) % n
        arrived(dgs.at[src], gs_sem.at[o], gr_sem.at[src])
    total_dg = dgs[0]
    for i in range(1, n):
        total_dg = total_dg + dgs[i]
    dg_ref[...] = total_dg
    for c in copies:
        c.wait_send()


def zeros(z, de_ref, first, rows, sem):
    zr = z.shape[0]
    z[...] = jnp.zeros_like(z)
    cs = [pltpu.make_async_copy(z, de_ref.at[pl.ds(first // 8 + i * zr, zr)], sem) for i in range(rows // (8 * zr))]
    for c in cs:
        c.start()
    return cs


def clear_and_list(n, rows, y_ref, ids_hbm, de_ref, x_ref, plan_ref, z, ids, found, table, plan, sem, x_sem, s_sem):
    load = pltpu.make_async_copy(ids_hbm, ids, s_sem.at[0])
    load.start()
    cs = zeros(z, de_ref, 0, rows, sem)
    out = pltpu.make_async_copy(y_ref.at[0], x_ref, x_sem)
    out.start()
    k, t = ids.shape
    h, kt = t // n, k * t
    vl = de_ref.shape[0] * 8
    lo = lax.axis_index("tp") * vl

    def reset(i, _):
        table[i] = -1
        return 0

    lax.fori_loop(0, table.shape[0], reset, 0, unroll=8)
    load.wait()
    cnt, used = jnp.int32(0), jnp.int32(0)
    for m in range(k):
        def find(i, cnt):
            v = ids[m, i]
            found[cnt] = i
            return cnt + ((v >= lo) & (v < lo + vl)).astype(jnp.int32)

        first = cnt
        cnt = lax.fori_loop(0, t, find, first, unroll=16)

        def one(c, used):
            i = found[c]
            v = ids[m, i] - lo
            b = lax.div(v, 8)
            s = table[b]
            fresh = (s < 0).astype(jnp.int32)
            s = jnp.where(s < 0, used, s)
            table[b] = s
            plan[c] = slab(i, m, k, h)
            plan[kt + c] = s * 16 + lax.rem(v, 8) * 2 + fresh
            plan[2 * kt + s] = b
            return used + fresh

        used = lax.fori_loop(first, cnt, one, used)
    plan[3 * kt] = cnt
    plan[3 * kt + 1] = used
    store = pltpu.make_async_copy(plan, plan_ref, s_sem.at[1])
    store.start()
    store.wait()
    out.wait()
    for c in cs:
        c.wait()


def project(parts, w_ref, du_ref, g_ref, u_ref, n_g, du_g, u_g, u_sem, emit):
    _, x0 = parts[0]
    k, h, d = x0.shape
    gf = g_ref[...].astype(F32).reshape(1, d)
    for p, (owner, x) in enumerate(parts):
        for m in range(k):
            base = p * (k * h) + m * h
            du_g[base:base + h] = du_ref[m, pl.ds(pl.multiple_of(owner * h, h), h)]
            for s in range(h // ROWS):
                xf = x[m, pl.ds(s * ROWS, ROWS)].astype(F32)
                rs = lax.rsqrt(jnp.mean(xf * xf, axis=-1, keepdims=True) + EPS)
                n_g[base + s * ROWS:base + (s + 1) * ROWS] = ((xf * rs) * gf).astype(BF16)
    u_g[...] = jnp.dot(n_g[...], w_ref[...], preferred_element_type=F32).astype(BF16)
    cs = []
    for p, (owner, _) in enumerate(parts):
        for m in range(k):
            cs.append(pltpu.make_async_copy(u_g.at[pl.ds(p * (k * h) + m * h, h)],
                                            u_ref.at[m, pl.ds(pl.multiple_of(owner * h, h), h)], u_sem))
    for c in cs:
        c.start()
    cw = 512
    for i in range(d // cw):
        emit(i, cw, lax.dot_general(n_g[:, i * cw:(i + 1) * cw], du_g[...], (((0,), (0,)), ((), ())),
                                    preferred_element_type=F32))
    return cs


def near_and_far(n):
    me = lax.axis_index("tp")
    chips = n // 2
    chip, core = me // 2, me % 2
    at = lambda off, c: ((chip + off) % chips) * 2 + c
    near = [at(0, core), at(chips - 1, core), at(1, core), at(0, 1 - core)]
    far = [at(2, core), at(chips - 1, 1 - core), at(1, 1 - core), at(2, 1 - core)]
    return near, far


def clear_rest(n, first, rows, y0, yl, yr, p0, w_ref, du_ref, g_ref, dg_in, de_in, de_ref, dg_ref, u_ref, dw_ref,
               z, n_g, du_g, u_g, sem, u_sem):
    del de_in
    cs = zeros(z, de_ref, first, rows, sem)
    dg_ref[...] = dg_in[...].reshape(dg_ref.shape)

    def emit(i, cw, v):
        dw_ref[i * cw:(i + 1) * cw] = v

    near, _ = near_and_far(n)
    us = project([(o, v.at[0]) for o, v in zip(near, (y0, yl, yr, p0))], w_ref, du_ref, g_ref, u_ref,
                 n_g, du_g, u_g, u_sem, emit)
    for c in us + cs:
        c.wait()


def finish(n, plan, y0, yl, yr, p0, xo, do, pl_, pr, pxo, pdo, w_ref, du_ref, g_ref, dw_in, u_in, de_in,
           u_ref, dw_ref, de_ref, dxf, acc, n_g, du_g, u_g, dw_s, sem, u_sem, w_sem):
    del de_in, u_in
    k, h, d = xo.shape
    kt = k * h * n
    near, far = near_and_far(n)
    dxs = list(zip(near, (y0.at[1], yl.at[1], yr.at[1], p0.at[1]))) + list(zip(far, (do, pl_.at[1], pr.at[1], pdo)))
    for owner, dx in dxs:
        for m in range(k):
            for s in range(h // ROWS):
                dxf[pl.ds(pl.multiple_of(owner * (k * h) + m * h + s * ROWS, ROWS), ROWS)] = dx[m, pl.ds(s * ROWS, ROWS)].astype(F32)

    sub = lax.broadcasted_iota(jnp.int32, (8, d), 0)
    cnt, used = plan[3 * kt], plan[3 * kt + 1]
    step = 4

    def drain(i, _):
        pltpu.make_async_copy(acc.at[0], de_ref.at[0], sem).wait()
        return 0

    def turn(q, _):
        @pl.when(q > 0)
        def _():
            lax.fori_loop(0, SLOTS, drain, 0)

        def some(b, _):
            todo = []
            for e in range(step):
                i = b * step + e
                c = jnp.minimum(i, cnt - 1)
                code = plan[kt + c]
                s = (code >> 4) - q * SLOTS
                s = jnp.where((i < cnt) & (s >= 0) & (s < SLOTS), s, SLOTS)
                todo.append((s, (code >> 1) & 7, (code & 1) == 1, dxf[pl.ds(plan[c], 1)]))
            for s, r, fresh, x in todo:
                old = jnp.where(fresh, jnp.zeros((8, d), F32), acc[s])
                acc[s] = old + jnp.where(sub == r, jnp.broadcast_to(x, (8, d)), 0.0)
            return 0

        lax.fori_loop(0, lax.div(cnt + step - 1, step), some, 0)

        def put(i, _):
            pltpu.make_async_copy(acc.at[i], de_ref.at[plan[2 * kt + q * SLOTS + i]], sem).start()
            return 0

        lax.fori_loop(0, jnp.minimum(used - q * SLOTS, SLOTS), put, 0)
        return 0

    turns = lax.div(used + SLOTS - 1, SLOTS)
    lax.fori_loop(0, turns, turn, 0)

    ws = []

    def emit(i, cw, v):
        rows = pl.ds(i * cw, cw)
        dw_s[rows] = dw_in[rows] + v
        ws.append(pltpu.make_async_copy(dw_s.at[rows], dw_ref.at[rows], w_sem))
        ws[-1].start()

    us = project(list(zip(far, (xo, pl_.at[0], pr.at[0], pxo))), w_ref, du_ref, g_ref, u_ref, n_g, du_g, u_g, u_sem, emit)
    for c in us + ws:
        c.wait()
    lax.fori_loop(0, used - jnp.maximum(turns - 1, 0) * SLOTS, drain, 0)


def solution(mesh):
    n = mesh.shape["tp"]
    chips = n // 2
    to_right = [(r, (r + 2) % n) for r in range(n)]
    to_left = [(r, (r + n - 2) % n) for r in range(n)]
    to_partner = [(r, r ^ 1) for r in range(n)]
    dma = pltpu.SemaphoreType.DMA

    def step(ids, emb, g, w, du, dres):
        k, t = ids.shape
        vl, d = emb.shape
        f = w.shape[1]
        h = t // n
        kt = k * t
        i32 = lambda *s: jax.ShapeDtypeStruct(s, jnp.int32)
        cost = lambda b: pl.CostEstimate(flops=0, bytes_accessed=b, transcendentals=0)

        rows = pl.pallas_call(
            functools.partial(lookup, n),
            out_shape=jax.ShapeDtypeStruct((kt, d), BF16),
            in_specs=[SMEM, HBM],
            out_specs=VMEM,
            scratch_shapes=[
                pltpu.VMEM((kt, 8, d), BF16), pltpu.VMEM((kt, d), F32), pltpu.SMEM((kt + 1,), jnp.int32),
                pltpu.SMEM((kt,), jnp.int32), pltpu.SMEM((kt,), jnp.int32), dma,
            ],
            compiler_params=pltpu.CompilerParams(vmem_limit_bytes=32 << 20),
            cost_estimate=cost(4 << 20),
            name="lookup",
        )(ids, emb.reshape(vl // 8, 8, d))

        y, dg = pl.pallas_call(
            functools.partial(exchange, n),
            out_shape=(jax.ShapeDtypeStruct((2, k, h, d), BF16), jax.ShapeDtypeStruct((1, d), F32)),
            in_specs=[VMEM] * 5,
            out_specs=(VMEM, VMEM),
            scratch_shapes=[
                pltpu.VMEM((n, k * h, d), BF16),
                pltpu.VMEM((chips, k * h, d), BF16),
                pltpu.VMEM((chips, k * h, d), BF16),
                pltpu.VMEM((chips, k * h, d), BF16),
                pltpu.VMEM((chips, k * h, d), F32),
                pltpu.VMEM((2, 3, h, d), BF16),
                pltpu.VMEM((2, 3, h, d), F32),
                pltpu.VMEM((k, h, d), F32),
                pltpu.VMEM((k, h, 128), F32),
                pltpu.VMEM((n, 1, d), F32),
                dma((chips,)), dma((chips,)), dma((chips,)), dma((chips,)),
                dma((2, 3)), dma((2, 3)), dma((2, 2 + h // ROWS)), dma((2, 2 + h // ROWS)),
                dma((n,)), dma((n,)),
            ],
            compiler_params=pltpu.CompilerParams(collective_id=0, has_side_effects=True, vmem_limit_bytes=28 << 20),
            name="exchange",
        )(rows.reshape(n, k * h, d), du, w, g, dres)

        def move(v, perm):
            return lax.ppermute(v, "tp", perm)

        yl = move(y, to_right)
        yr = move(y, to_left)
        py = move(y, to_partner)
        xo = move(yl[0], to_right)
        do = move(yr[1], to_left)
        pyl = move(yl, to_partner)
        pyr = move(yr, to_partner)
        pxo = move(xo, to_partner)
        pdo = move(do, to_partner)

        zr = 16
        split = (vl * 5 // 8) // (8 * zr) * (8 * zr)
        de_shape = jax.ShapeDtypeStruct((vl // 8, 8, d), F32)
        u_shape = jax.ShapeDtypeStruct((k, t, f), BF16)
        dw_shape = jax.ShapeDtypeStruct((d, f), F32)
        size = 3 * kt + 128
        some = n // 2 * k * h
        smem = lambda *s: pltpu.SMEM(s, jnp.int32)
        group = [pltpu.VMEM((some, d), BF16), pltpu.VMEM((some, f), BF16), pltpu.VMEM((some, f), BF16)]
        de, x, plan = pl.pallas_call(
            functools.partial(clear_and_list, n, split),
            out_shape=(de_shape, jax.ShapeDtypeStruct((k, h, d), BF16), i32(size)),
            in_specs=[VMEM, ANY],
            out_specs=(ANY, ANY, ANY),
            scratch_shapes=[pltpu.VMEM((zr, 8, d), F32), smem(k, t), smem(kt + 1), smem(vl // 8), smem(size),
                            dma, dma, dma((2,))],
            compiler_params=pltpu.CompilerParams(vmem_limit_bytes=8 << 20),
            cost_estimate=cost(split * d * 4),
            name="clear0",
        )(y, ids)
        de, dgf, u, dwa = pl.pallas_call(
            functools.partial(clear_rest, n, split, vl - split),
            out_shape=(de_shape, jax.ShapeDtypeStruct((d,), F32), u_shape, dw_shape),
            in_specs=[VMEM] * 8 + [ANY], out_specs=(ANY, VMEM, ANY, VMEM),
            input_output_aliases={8: 0},
            scratch_shapes=[pltpu.VMEM((zr, 8, d), F32)] + group + [dma, dma],
            compiler_params=pltpu.CompilerParams(vmem_limit_bytes=12 << 20),
            cost_estimate=cost((vl - split) * d * 4),
            name="clear1",
        )(y, yl, yr, py, w, du, g, dg, de)

        u, dw, de = pl.pallas_call(
            functools.partial(finish, n),
            out_shape=(u_shape, dw_shape, de_shape),
            in_specs=[SMEM] + [VMEM] * 14 + [ANY, ANY],
            out_specs=(ANY, ANY, ANY),
            input_output_aliases={15: 0, 16: 2},
            scratch_shapes=[pltpu.VMEM((kt, d), F32), pltpu.VMEM((SLOTS + 1, 8, d), F32)] + group
                           + [pltpu.VMEM((d, f), F32), dma, dma, dma],
            compiler_params=pltpu.CompilerParams(vmem_limit_bytes=28 << 20),
            name="finish",
        )(plan, y, yl, yr, py, xo, do, pyl, pyr, pxo, pdo, w, du, g, dwa, u, de)
        return u, x, de.reshape(vl, d), dw, dgf

    return jax.shard_map(
        step,
        mesh=mesh,
        in_specs=(P("dp", None), P("tp", None), P(None), P(None, "tp"), P("dp", None, "tp"), P("dp", "tp", None)),
        out_specs=(P("dp", None, "tp"), P("dp", "tp", None), P(("dp", "tp"), None), P(None, ("dp", "tp")), P("dp")),
        check_vma=False,
    )
```

```python
import functools

import jax
import jax.numpy as jnp
from jax import lax
from jax.experimental import pallas as pl
from jax.experimental.pallas import tpu as pltpu
from jax.sharding import PartitionSpec as P


EPS = 1e-6
MESH = pl.DeviceIdType.MESH
VMEM = pl.BlockSpec(memory_space=pltpu.VMEM)
SMEM = pl.BlockSpec(memory_space=pltpu.SMEM)
ANY = pl.BlockSpec(memory_space=pl.ANY)
HBM = pl.BlockSpec(memory_space=pltpu.HBM)
F32 = jnp.float32
BF16 = jnp.bfloat16
ROWS = 16
SLOTS = 128


def slab(i, m, k, h):
    return lax.div(i, h) * (k * h) + m * h + lax.rem(i, h)


def ring_places(n):
    me = lax.axis_index("tp")
    chips = n // 2
    return me, me // 2, me % 2, chips


def parts(n, du_ref, w_ref, mine_ref, other_ref, du_g):
    _, chip, core, chips = ring_places(n)
    k, t, _ = du_ref.shape
    h = t // n
    half = chips * k * h
    for side in range(2):
        for j in range(chips):
            owner = ((chip + j) % chips) * 2 + (core if side == 0 else 1 - core)
            for m in range(k):
                base = side * half + j * (k * h) + m * h
                du_g[base:base + h] = du_ref[m, pl.ds(pl.multiple_of(owner * h, h), h)]
    cw = 256

    def cols(i, _):
        c0 = pl.multiple_of(i * cw, cw)
        v = lax.dot_general(du_g[...], w_ref[pl.ds(c0, cw), :], (((1,), (1,)), ((), ())), preferred_element_type=F32)
        v = v.astype(BF16)
        mine_ref[:, :, pl.ds(c0, cw)] = v[:half].reshape(chips, k * h, cw)
        other_ref[:, :, pl.ds(c0, cw)] = v[half:].reshape(chips, k * h, cw)
        return 0

    lax.fori_loop(0, w_ref.shape[0] // cw, cols, 0)


def lookup(n, ids_ref, emb_ref, mine_ref, other_ref, buf, pf, found, at_s, row_s, sem):
    me, chip, core, chips = ring_places(n)
    k, t = ids_ref.shape
    h = t // n
    d = emb_ref.shape[2]
    vl = emb_ref.shape[0] * 8
    lo = me * vl
    half = chips * k * h

    cnt = jnp.int32(0)
    for m in range(k):
        def find(i, cnt):
            v = ids_ref[m, i]
            found[cnt] = i
            return cnt + ((v >= lo) & (v < lo + vl)).astype(jnp.int32)

        first = cnt
        cnt = lax.fori_loop(0, t, find, first, unroll=16)

        def fetch(c, _):
            i = found[c]
            v = ids_ref[m, i] - lo
            pltpu.make_async_copy(emb_ref.at[lax.div(v, 8)], buf.at[c], sem).start()
            owner = lax.div(i, h)
            side = jnp.where(lax.rem(owner, 2) == core, 0, half)
            j = lax.rem(lax.div(owner, 2) - chip + chips, chips)
            at_s[c] = side + j * (k * h) + m * h + lax.rem(i, h)
            row_s[c] = lax.rem(v, 8)
            return 0

        lax.fori_loop(first, cnt, fetch, 0)

    pf[...] = jnp.zeros_like(pf)
    sub = lax.broadcasted_iota(jnp.int32, (8, d), 0)

    def wait(i, _):
        pltpu.make_async_copy(emb_ref.at[0], buf.at[0], sem).wait()
        return 0

    lax.fori_loop(0, cnt, wait, 0)
    step = 4

    def place(q, _):
        rows = []
        for u in range(step):
            i = jnp.minimum(q * step + u, cnt - 1)
            x8 = buf[i].astype(F32)
            rows.append((at_s[i], jnp.sum(jnp.where(sub == row_s[i], x8, 0.0), axis=0, keepdims=True)))
        for at, x in rows:
            pf[pl.ds(at, 1)] = x
        return 0

    lax.fori_loop(0, lax.div(cnt + step - 1, step), place, 0)

    def pack(i, _):
        r0 = pl.multiple_of(i * ROWS, ROWS)
        mine_ref[pl.ds(r0, ROWS)] = pf[pl.ds(r0, ROWS)].astype(BF16)
        other_ref[pl.ds(r0, ROWS)] = pf[pl.ds(half + r0, ROWS)].astype(BF16)
        return 0

    lax.fori_loop(0, half // ROWS, pack, 0)


def fold(h, a_ref, b_ref, right_ref, left_ref, next_ref, prev_ref, own_ref):
    def put(dst, j, m):
        rows = pl.ds(m * h, h)
        dst[...] = a_ref[j, rows].astype(dst.dtype) + b_ref[j, rows].astype(dst.dtype)

    put(right_ref.at[0], 2, 0)
    put(left_ref.at[0], 2, 1)
    put(right_ref.at[1], 1, 1)
    put(left_ref.at[1], 3, 0)
    put(next_ref, 1, 0)
    put(prev_ref, 3, 1)
    put(own_ref.at[0], 0, 0)
    put(own_ref.at[1], 0, 1)


def relay(xn, xp, xl, xr, dn, dp, dl, dr, xn_ref, xp_ref, dn_ref, dp_ref):
    xn_ref[...] = xn[...] + xl[0]
    xp_ref[...] = xp[...] + xr[0]
    dn_ref[...] = dn[...] + dl[0]
    dp_ref[...] = dp[...] + dr[0]


def zeros(z, de_ref, first, rows, sem):
    zr = z.shape[0]
    z[...] = jnp.zeros_like(z)
    cs = [pltpu.make_async_copy(z, de_ref.at[pl.ds(first // 8 + i * zr, zr)], sem) for i in range(rows // (8 * zr))]
    for c in cs:
        c.start()
    return cs


def clear_and_list(n, rows, ids_hbm, de_ref, plan_ref, z, ids, found, table, plan, sem, s_sem):
    load = pltpu.make_async_copy(ids_hbm, ids, s_sem.at[0])
    load.start()
    cs = zeros(z, de_ref, 0, rows, sem)
    k, t = ids.shape
    h, kt = t // n, k * t
    vl = de_ref.shape[0] * 8
    lo = lax.axis_index("tp") * vl

    def reset(i, _):
        table[i] = -1
        return 0

    lax.fori_loop(0, table.shape[0], reset, 0, unroll=8)
    load.wait()
    cnt, used = jnp.int32(0), jnp.int32(0)
    for m in range(k):
        def find(i, cnt):
            v = ids[m, i]
            found[cnt] = i
            return cnt + ((v >= lo) & (v < lo + vl)).astype(jnp.int32)

        first = cnt
        cnt = lax.fori_loop(0, t, find, first, unroll=16)

        def one(c, used):
            i = found[c]
            v = ids[m, i] - lo
            b = lax.div(v, 8)
            s = table[b]
            fresh = (s < 0).astype(jnp.int32)
            s = jnp.where(s < 0, used, s)
            table[b] = s
            plan[c] = slab(i, m, k, h)
            plan[kt + c] = s * 16 + lax.rem(v, 8) * 2 + fresh
            plan[2 * kt + s] = b
            return used + fresh

        used = lax.fori_loop(first, cnt, one, used)
    plan[3 * kt] = cnt
    plan[3 * kt + 1] = used
    store = pltpu.make_async_copy(plan, plan_ref, s_sem.at[1])
    store.start()
    store.wait()
    for c in cs:
        c.wait()


def clear_rest(first, rows, de_in, de_ref, z, sem):
    del de_in
    for c in zeros(z, de_ref, first, rows, sem):
        c.wait()


def spread(n, x0, xl1, xr1, xl2, xr2, d0, dl1, dr1, dl2, dr2, g_ref, dres_ref, w_ref, du_ref,
           dx_all, x_ref, u_ref, dw_ref, dg_ref, x_all, nh_s, rs_s, dgs, n_g, du_g, s_sem, r_sem, gs_sem, gr_sem):
    me, chip, core, chips = ring_places(n)
    k, h, d = dres_ref.shape
    at = lambda off, c: ((chip + off) % chips) * 2 + c
    left, right, far = at(chips - 1, core), at(1, core), at(2, core)
    partner, p_left, p_right, p_far = at(0, 1 - core), at(chips - 1, 1 - core), at(1, 1 - core), at(2, 1 - core)
    near = (me, left, right, partner)
    rest = (far, p_left, p_right, p_far)

    barrier = pltpu.get_barrier_semaphore()
    for o in range(1, n):
        pl.semaphore_signal(barrier, inc=1, device_id={"tp": (me + o) % n}, device_id_type=MESH)

    gf = g_ref[...].astype(F32).reshape(1, d)
    pieces = h // ROWS
    sides = ((xr1, xl2, dr1, dl2), (xl1, xr2, dl1, dr2))
    for m in range(k):
        xa, xb, _, _ = sides[m]
        for i in range(pieces):
            rows = pl.ds(i * ROWS, ROWS)
            x = x0[m, rows] + xa[1, rows] + xb[rows]
            x_ref[m, rows] = x
            x_all[me, m, rows] = x
            xf = x.astype(F32)
            rs = lax.rsqrt(jnp.mean(xf * xf, axis=-1, keepdims=True) + EPS)
            nh_s[m, rows] = xf * rs
            rs_s[m, rows] = jnp.broadcast_to(rs, (ROWS, rs_s.shape[-1]))
    pl.semaphore_wait(barrier, n - 1)

    copies = []

    def send(src, dst, ss, rs, to):
        c = pltpu.make_async_remote_copy(src_ref=src, dst_ref=dst, send_sem=ss, recv_sem=rs,
                                         device_id={"tp": to}, device_id_type=MESH)
        c.start()
        copies.append(c)

    def arrived(dst, ss, rs):
        pltpu.make_async_remote_copy(src_ref=dst, dst_ref=dst, send_sem=ss, recv_sem=rs,
                                     device_id={"tp": partner}, device_id_type=MESH).wait_recv()

    def own(kind, ref):
        for slot, (to, rel) in enumerate(((right, 1), (left, 2), (partner, 0))):
            send(ref.at[me], ref.at[me], s_sem.at[kind, slot], r_sem.at[kind, rel], to)

    def got(kind, rel, view):
        arrived(view, s_sem.at[kind, rel], r_sem.at[kind, rel])

    def onward(kind, ref):
        got(kind, 1, ref.at[left])
        send(ref.at[left, 0], ref.at[left, 0], s_sem.at[kind, 3], r_sem.at[kind, 5], right)
        got(kind, 2, ref.at[right])
        send(ref.at[right, 1], ref.at[right, 1], s_sem.at[kind, 4], r_sem.at[kind, 6], left)
        send(ref.at[left], ref.at[left], s_sem.at[kind, 5], r_sem.at[kind, 3], partner)
        send(ref.at[right], ref.at[right], s_sem.at[kind, 6], r_sem.at[kind, 4], partner)
        got(kind, 0, ref.at[partner])

    def across(kind, ref):
        for m in range(2):
            got(kind, 5 + m, ref.at[far, m])
            send(ref.at[far, m], ref.at[far, m], s_sem.at[kind, 7 + m], r_sem.at[kind, 7 + m], partner)
        got(kind, 3, ref.at[p_left])
        got(kind, 4, ref.at[p_right])

    def last(kind, ref):
        for m in range(2):
            got(kind, 7 + m, ref.at[p_far, m])

    own(0, x_all)

    dg = jnp.zeros((1, d), F32)
    for m in range(k):
        _, _, da, db = sides[m]
        for i in range(pieces):
            rows = pl.ds(i * ROWS, ROWS)
            dn = d0[m, rows] + da[1, rows] + db[rows]
            nh = nh_s[m, rows]
            dg = dg + jnp.sum(dn * nh, axis=0, keepdims=True)
            gdn = gf * dn
            dxn = rs_s[m, rows, :1] * (gdn - nh * jnp.mean(nh * gdn, axis=-1, keepdims=True))
            dx_all[me, m, rows] = (dres_ref[m, rows].astype(F32) + dxn).astype(BF16)
    dgs[me] = dg
    own(1, dx_all)
    for o in range(1, n):
        send(dgs.at[me], dgs.at[me], gs_sem.at[o], gr_sem.at[me], (me + o) % n)

    def project(owners, add):
        for p, owner in enumerate(owners):
            for m in range(k):
                base = p * (k * h) + m * h
                du_g[base:base + h] = du_ref[m, pl.ds(pl.multiple_of(owner * h, h), h)]
                for i in range(pieces):
                    xf = x_all[owner, m, pl.ds(i * ROWS, ROWS)].astype(F32)
                    rs = lax.rsqrt(jnp.mean(xf * xf, axis=-1, keepdims=True) + EPS)
                    n_g[base + i * ROWS:base + (i + 1) * ROWS] = ((xf * rs) * gf).astype(BF16)
        u = jnp.dot(n_g[...], w_ref[...], preferred_element_type=F32).astype(BF16)
        for p, owner in enumerate(owners):
            for m in range(k):
                base = p * (k * h) + m * h
                u_ref[m, pl.ds(pl.multiple_of(owner * h, h), h)] = u[base:base + h]
        cw = 512
        for i in range(d // cw):
            v = lax.dot_general(n_g[:, i * cw:(i + 1) * cw], du_g[...], (((0,), (0,)), ((), ())),
                                preferred_element_type=F32)
            rows = slice(i * cw, (i + 1) * cw)
            dw_ref[rows] = dw_ref[rows] + v if add else v

    onward(0, x_all)
    project(near, False)
    onward(1, dx_all)
    across(0, x_all)
    last(0, x_all)
    project(rest, True)
    across(1, dx_all)
    last(1, dx_all)

    for o in range(1, n):
        src = (me + o) % n
        arrived(dgs.at[src], gs_sem.at[o], gr_sem.at[src])
    total_dg = dgs[0]
    for i in range(1, n):
        total_dg = total_dg + dgs[i]
    dg_ref[...] = total_dg
    for c in copies:
        c.wait_send()


def finish(plan, dx_all, x_in, u_in, dw_in, dg_in, de_in, x_ref, u_ref, dw_ref, dg_ref, de_ref, dxf, acc, sem, o_sem):
    del de_in
    outs = [pltpu.make_async_copy(src, dst, o_sem.at[i])
            for i, (src, dst) in enumerate(((dw_in, dw_ref), (u_in, u_ref), (x_in, x_ref)))]
    for c in outs:
        c.start()
    dg_ref[...] = dg_in[...].reshape(dg_ref.shape)
    n, k, h, d = dx_all.shape
    kt = k * h * n

    def widen(i, _):
        for m in range(k):
            for s in range(h // ROWS):
                dxf[pl.ds(pl.multiple_of(i * (k * h) + m * h + s * ROWS, ROWS), ROWS)] = dx_all[i, m, pl.ds(s * ROWS, ROWS)].astype(F32)
        return 0

    lax.fori_loop(0, n, widen, 0)

    sub = lax.broadcasted_iota(jnp.int32, (8, d), 0)
    cnt, used = plan[3 * kt], plan[3 * kt + 1]
    step = 4

    def drain(i, _):
        pltpu.make_async_copy(acc.at[0], de_ref.at[0], sem).wait()
        return 0

    def turn(q, _):
        @pl.when(q > 0)
        def _():
            lax.fori_loop(0, SLOTS, drain, 0)

        def some(b, _):
            todo = []
            for e in range(step):
                i = b * step + e
                c = jnp.minimum(i, cnt - 1)
                code = plan[kt + c]
                s = (code >> 4) - q * SLOTS
                s = jnp.where((i < cnt) & (s >= 0) & (s < SLOTS), s, SLOTS)
                todo.append((s, (code >> 1) & 7, (code & 1) == 1, dxf[pl.ds(plan[c], 1)]))
            for s, r, fresh, x in todo:
                old = jnp.where(fresh, jnp.zeros((8, d), F32), acc[s])
                acc[s] = old + jnp.where(sub == r, jnp.broadcast_to(x, (8, d)), 0.0)
            return 0

        lax.fori_loop(0, lax.div(cnt + step - 1, step), some, 0)

        def put(i, _):
            pltpu.make_async_copy(acc.at[i], de_ref.at[plan[2 * kt + q * SLOTS + i]], sem).start()
            return 0

        lax.fori_loop(0, jnp.minimum(used - q * SLOTS, SLOTS), put, 0)
        return 0

    turns = lax.div(used + SLOTS - 1, SLOTS)
    lax.fori_loop(0, turns, turn, 0)

    for c in outs:
        c.wait()
    lax.fori_loop(0, used - jnp.maximum(turns - 1, 0) * SLOTS, drain, 0)


def solution(mesh):
    n = mesh.shape["tp"]
    chips = n // 2
    to_right = [(r, (r + 2) % n) for r in range(n)]
    to_left = [(r, (r + n - 2) % n) for r in range(n)]
    to_partner = [(r, r ^ 1) for r in range(n)]
    dma = pltpu.SemaphoreType.DMA

    def step(ids, emb, g, w, du, dres):
        k, t = ids.shape
        vl, d = emb.shape
        f = w.shape[1]
        h = t // n
        kt = k * t
        shape = jax.ShapeDtypeStruct
        i32 = lambda *s: shape(s, jnp.int32)
        smem = lambda *s: pltpu.SMEM(s, jnp.int32)
        cost = lambda b: pl.CostEstimate(flops=0, bytes_accessed=b, transcendentals=0)
        limit = lambda mib, **kw: pltpu.CompilerParams(vmem_limit_bytes=mib << 20, **kw)

        def move(v, perm):
            return lax.ppermute(v, "tp", perm)

        side = shape((chips, k * h, d), BF16)
        dm, do = pl.pallas_call(
            functools.partial(parts, n),
            out_shape=(side, side), in_specs=[VMEM] * 2, out_specs=(VMEM, VMEM),
            scratch_shapes=[pltpu.VMEM((kt, f), BF16)],
            compiler_params=limit(8), cost_estimate=cost(4 << 20), name="parts",
        )(du, w)
        dp = move(do, to_partner)

        flat = shape((kt // 2, d), BF16)
        xm, xo = pl.pallas_call(
            functools.partial(lookup, n),
            out_shape=(flat, flat), in_specs=[SMEM, HBM], out_specs=(VMEM, VMEM),
            scratch_shapes=[pltpu.VMEM((kt, 8, d), BF16), pltpu.VMEM((kt, d), F32), smem(kt + 1), smem(kt), smem(kt), dma],
            compiler_params=limit(32), cost_estimate=cost(16 << 20), name="lookup",
        )(ids, emb.reshape(vl // 8, 8, d))
        xp = move(xo.reshape(chips, k * h, d), to_partner)

        def fold_of(a, b, dtype):
            two, one = shape((2, h, d), dtype), shape((h, d), dtype)
            return pl.pallas_call(
                functools.partial(fold, h),
                out_shape=(two, two, one, one, two), in_specs=[VMEM] * 2, out_specs=(VMEM,) * 5,
                compiler_params=limit(8), cost_estimate=cost(2 << 20),
            )(a, b)

        d_r, d_l, d_n, d_p, d0 = fold_of(dm, dp, F32)
        x_r, x_l, x_n, x_p, x0 = fold_of(xm.reshape(chips, k * h, d), xp, BF16)
        dl1 = move(d_r, to_right)
        dr1 = move(d_l, to_left)
        xl1 = move(x_r, to_right)
        xr1 = move(x_l, to_left)

        zr = 16
        split = (vl * 10 // 16) // (8 * zr) * (8 * zr)
        de_shape = shape((vl // 8, 8, d), F32)
        size = 3 * kt + 128
        de, plan = pl.pallas_call(
            functools.partial(clear_and_list, n, split),
            out_shape=(de_shape, i32(size)), in_specs=[ANY], out_specs=(ANY, ANY),
            scratch_shapes=[pltpu.VMEM((zr, 8, d), F32), smem(k, t), smem(kt + 1), smem(vl // 8), smem(size),
                            dma, dma((2,))],
            compiler_params=limit(8), cost_estimate=cost(split * d * 4), name="clear0",
        )(ids)

        half_x, half_d = shape((h, d), BF16), shape((h, d), F32)
        x_n, x_p, d_n, d_p = pl.pallas_call(
            relay, out_shape=(half_x, half_x, half_d, half_d), in_specs=[VMEM] * 8, out_specs=(VMEM,) * 4,
            compiler_params=limit(8), cost_estimate=cost(2 << 20), name="relay",
        )(x_n, x_p, xl1, xr1, d_n, d_p, dl1, dr1)
        dl2 = move(d_n, to_right)
        dr2 = move(d_p, to_left)
        xl2 = move(x_n, to_right)
        xr2 = move(x_p, to_left)

        de = pl.pallas_call(
            functools.partial(clear_rest, split, vl - split),
            out_shape=de_shape, in_specs=[ANY], out_specs=ANY, input_output_aliases={0: 0},
            scratch_shapes=[pltpu.VMEM((zr, 8, d), F32), dma],
            compiler_params=limit(8), cost_estimate=cost((vl - split) * d * 4), name="clear1",
        )(de)

        tok, u_s, dw_s = shape((k, h, d), BF16), shape((k, t, f), BF16), shape((d, f), F32)
        some = kt // 2
        dx_all, x, u, dw, dg = pl.pallas_call(
            functools.partial(spread, n),
            out_shape=(shape((n, k, h, d), BF16), tok, u_s, dw_s, shape((1, d), F32)),
            in_specs=[VMEM] * 14, out_specs=(VMEM,) * 5,
            scratch_shapes=[pltpu.VMEM((n, k, h, d), BF16), pltpu.VMEM((k, h, d), F32), pltpu.VMEM((k, h, 128), F32),
                            pltpu.VMEM((n, 1, d), F32), pltpu.VMEM((some, d), BF16), pltpu.VMEM((some, f), BF16),
                            dma((2, 9)), dma((2, 9)), dma((n,)), dma((n,))],
            compiler_params=limit(24, collective_id=0, has_side_effects=True), name="spread",
        )(x0, xl1, xr1, xl2, xr2, d0, dl1, dr1, dl2, dr2, g, dres, w, du)

        x, u, dw, dg, de = pl.pallas_call(
            finish,
            out_shape=(tok, u_s, dw_s, shape((d,), F32), de_shape),
            in_specs=[SMEM] + [VMEM] * 5 + [ANY], out_specs=(ANY, ANY, ANY, VMEM, ANY),
            input_output_aliases={6: 4},
            scratch_shapes=[pltpu.VMEM((kt, d), F32), pltpu.VMEM((SLOTS + 1, 8, d), F32), dma, dma((3,))],
            compiler_params=limit(24), name="finish",
        )(plan, dx_all, x, u, dw, dg, de)
        return u, x, de.reshape(vl, d), dw, dg

    return jax.shard_map(
        step,
        mesh=mesh,
        in_specs=(P("dp", None), P("tp", None), P(None), P(None, "tp"), P("dp", None, "tp"), P("dp", "tp", None)),
        out_specs=(P("dp", None, "tp"), P("dp", "tp", None), P(("dp", "tp"), None), P(None, ("dp", "tp")), P("dp")),
        check_vma=False,
    )
```

```python
import functools

import jax
import jax.numpy as jnp
from jax import lax
from jax.experimental import pallas as pl
from jax.experimental.pallas import tpu as pltpu
from jax.sharding import PartitionSpec as P


EPS = 1e-6
MESH = pl.DeviceIdType.MESH
VMEM = pl.BlockSpec(memory_space=pltpu.VMEM)
SMEM = pl.BlockSpec(memory_space=pltpu.SMEM)
ANY = pl.BlockSpec(memory_space=pl.ANY)
HBM = pl.BlockSpec(memory_space=pltpu.HBM)
F32 = jnp.float32
BF16 = jnp.bfloat16
ROWS = 16
SLOTS = 128


def slab(i, m, k, h):
    return lax.div(i, h) * (k * h) + m * h + lax.rem(i, h)


def ring_places(n):
    me = lax.axis_index("tp")
    chips = n // 2
    return me, me // 2, me % 2, chips


def parts(n, du_ref, w_ref, after_ref, mine_ref, other_ref, du_g):
    del after_ref
    _, chip, core, chips = ring_places(n)
    k, t, _ = du_ref.shape
    h = t // n
    half = chips * k * h
    for side in range(2):
        for j in range(chips):
            owner = ((chip + j) % chips) * 2 + (core if side == 0 else 1 - core)
            for m in range(k):
                base = side * half + j * (k * h) + m * h
                du_g[base:base + h] = du_ref[m, pl.ds(pl.multiple_of(owner * h, h), h)]
    cw = 256

    def cols(i, _):
        c0 = pl.multiple_of(i * cw, cw)
        v = lax.dot_general(du_g[...], w_ref[pl.ds(c0, cw), :], (((1,), (1,)), ((), ())), preferred_element_type=F32)
        v = v.astype(BF16)
        mine_ref[:, :, pl.ds(c0, cw)] = v[:half].reshape(chips, k * h, cw)
        other_ref[:, :, pl.ds(c0, cw)] = v[half:].reshape(chips, k * h, cw)
        return 0

    lax.fori_loop(0, w_ref.shape[0] // cw, cols, 0)


def lookup(n, ids_ref, emb_ref, mine_ref, other_ref, buf, pf, found, at_s, row_s, sem):
    me, chip, core, chips = ring_places(n)
    k, t = ids_ref.shape
    h = t // n
    d = emb_ref.shape[2]
    vl = emb_ref.shape[0] * 8
    lo = me * vl
    half = chips * k * h

    cnt = jnp.int32(0)
    for m in range(k):
        def find(i, cnt):
            v = ids_ref[m, i]
            found[cnt] = i
            return cnt + ((v >= lo) & (v < lo + vl)).astype(jnp.int32)

        first = cnt
        cnt = lax.fori_loop(0, t, find, first, unroll=16)

        def fetch(c, _):
            i = found[c]
            v = ids_ref[m, i] - lo
            pltpu.make_async_copy(emb_ref.at[lax.div(v, 8)], buf.at[c], sem).start()
            owner = lax.div(i, h)
            side = jnp.where(lax.rem(owner, 2) == core, 0, half)
            j = lax.rem(lax.div(owner, 2) - chip + chips, chips)
            at_s[c] = side + j * (k * h) + m * h + lax.rem(i, h)
            row_s[c] = lax.rem(v, 8)
            return 0

        lax.fori_loop(first, cnt, fetch, 0)

    pf[...] = jnp.zeros_like(pf)
    sub = lax.broadcasted_iota(jnp.int32, (8, d), 0)

    def wait(i, _):
        pltpu.make_async_copy(emb_ref.at[0], buf.at[0], sem).wait()
        return 0

    lax.fori_loop(0, cnt, wait, 0)
    step = 4

    def place(q, _):
        rows = []
        for u in range(step):
            i = jnp.minimum(q * step + u, cnt - 1)
            at = at_s[i]
            to = at & 7
            rows.append((at >> 3, to, pltpu.roll(buf[i].astype(F32), (to - row_s[i]) & 7, 0)))
        for block, to, x in rows:
            pf[block] = jnp.where(sub == to, x, pf[block])
        return 0

    lax.fori_loop(0, lax.div(cnt + step - 1, step), place, 0)

    def pack(i, _):
        r0 = pl.multiple_of(i * ROWS, ROWS)
        b0 = pl.multiple_of(i * (ROWS // 8), ROWS // 8)
        for dst, first in ((mine_ref, 0), (other_ref, half // 8)):
            dst[pl.ds(r0, ROWS)] = pf[pl.ds(first + b0, ROWS // 8)].reshape(ROWS, d).astype(BF16)
        return 0

    lax.fori_loop(0, half // ROWS, pack, 0)


def fold(h, a_ref, b_ref, right_ref, left_ref, next_ref, prev_ref, own_ref):
    def put(dst, j, m):
        rows = pl.ds(m * h, h)
        dst[...] = a_ref[j, rows].astype(dst.dtype) + b_ref[j, rows].astype(dst.dtype)

    put(right_ref.at[0], 2, 0)
    put(left_ref.at[0], 2, 1)
    put(right_ref.at[1], 1, 1)
    put(left_ref.at[1], 3, 0)
    put(next_ref, 1, 0)
    put(prev_ref, 3, 1)
    put(own_ref.at[0], 0, 0)
    put(own_ref.at[1], 0, 1)


def relay(nxt, prv, from_left, from_right, nxt_ref, prv_ref):
    nxt_ref[...] = nxt[...] + from_left[0]
    prv_ref[...] = prv[...] + from_right[0]


def zeros(z, de_ref, first, rows, sem):
    zr = z.shape[0]
    z[...] = jnp.zeros_like(z)
    cs = [pltpu.make_async_copy(z, de_ref.at[pl.ds(first // 8 + i * zr, zr)], sem) for i in range(rows // (8 * zr))]
    for c in cs:
        c.start()
    return cs


def clear_and_list(n, rows, ids_hbm, de_ref, plan_ref, z, ids, found, table, plan, sem, s_sem):
    load = pltpu.make_async_copy(ids_hbm, ids, s_sem.at[0])
    load.start()
    cs = zeros(z, de_ref, 0, rows, sem)
    k, t = ids.shape
    h, kt = t // n, k * t
    vl = de_ref.shape[0] * 8
    lo = lax.axis_index("tp") * vl

    def reset(i, _):
        table[i] = -1
        return 0

    lax.fori_loop(0, table.shape[0], reset, 0, unroll=8)
    load.wait()
    cnt, used = jnp.int32(0), jnp.int32(0)
    for m in range(k):
        def find(i, cnt):
            v = ids[m, i]
            found[cnt] = i
            return cnt + ((v >= lo) & (v < lo + vl)).astype(jnp.int32)

        first = cnt
        cnt = lax.fori_loop(0, t, find, first, unroll=16)

        def one(c, used):
            i = found[c]
            v = ids[m, i] - lo
            b = lax.div(v, 8)
            s = table[b]
            fresh = (s < 0).astype(jnp.int32)
            s = jnp.where(s < 0, used, s)
            table[b] = s
            plan[c] = slab(i, m, k, h)
            plan[kt + c] = s * 16 + lax.rem(v, 8) * 2 + fresh
            plan[2 * kt + s] = b
            return used + fresh

        used = lax.fori_loop(first, cnt, one, used)
    plan[3 * kt] = cnt
    plan[3 * kt + 1] = used
    store = pltpu.make_async_copy(plan, plan_ref, s_sem.at[1])
    store.start()
    store.wait()
    for c in cs:
        c.wait()


def clear_rest(first, rows, de_in, de_ref, z, sem):
    del de_in
    for c in zeros(z, de_ref, first, rows, sem):
        c.wait()


def spread(n, x0, xl1, xr1, xl2, xr2, d0, dl1, dr1, dl2, dr2, g_ref, dres_ref, w_ref, du_ref,
           dx_all, x_ref, u_ref, dw_ref, dg_ref, x_all, nh_s, rs_s, dgs, n_g, du_g, s_sem, r_sem, gs_sem, gr_sem):
    me, chip, core, chips = ring_places(n)
    k, h, d = dres_ref.shape
    at = lambda off, c: ((chip + off) % chips) * 2 + c
    left, right, far = at(chips - 1, core), at(1, core), at(2, core)
    partner, p_left, p_right, p_far = at(0, 1 - core), at(chips - 1, 1 - core), at(1, 1 - core), at(2, 1 - core)
    near = (me, left, right, partner)
    rest = (far, p_left, p_right, p_far)

    barrier = pltpu.get_barrier_semaphore()
    for o in range(1, n):
        pl.semaphore_signal(barrier, inc=1, device_id={"tp": (me + o) % n}, device_id_type=MESH)

    gf = g_ref[...].astype(F32).reshape(1, d)
    pieces = h // ROWS
    sides = ((xr1, xl2, dr1, dl2), (xl1, xr2, dl1, dr2))
    for m in range(k):
        xa, xb, _, _ = sides[m]
        for i in range(pieces):
            rows = pl.ds(i * ROWS, ROWS)
            x = x0[m, rows] + xa[1, rows] + xb[rows]
            x_ref[m, rows] = x
            x_all[me, m, rows] = x
            xf = x.astype(F32)
            rs = lax.rsqrt(jnp.mean(xf * xf, axis=-1, keepdims=True) + EPS)
            nh_s[m, rows] = xf * rs
            rs_s[m, rows] = jnp.broadcast_to(rs, (ROWS, rs_s.shape[-1]))
    pl.semaphore_wait(barrier, n - 1)

    copies = []

    def send(src, dst, ss, rs, to):
        c = pltpu.make_async_remote_copy(src_ref=src, dst_ref=dst, send_sem=ss, recv_sem=rs,
                                         device_id={"tp": to}, device_id_type=MESH)
        c.start()
        copies.append(c)

    def arrived(dst, ss, rs):
        pltpu.make_async_remote_copy(src_ref=dst, dst_ref=dst, send_sem=ss, recv_sem=rs,
                                     device_id={"tp": partner}, device_id_type=MESH).wait_recv()

    def own(kind, ref):
        for slot, (to, rel) in enumerate(((right, 1), (left, 2), (partner, 0))):
            send(ref.at[me], ref.at[me], s_sem.at[kind, slot], r_sem.at[kind, rel], to)

    def got(kind, rel, view):
        arrived(view, s_sem.at[kind, rel], r_sem.at[kind, rel])

    def onward(kind, ref):
        got(kind, 1, ref.at[left])
        send(ref.at[left, 0], ref.at[left, 0], s_sem.at[kind, 3], r_sem.at[kind, 5], right)
        got(kind, 2, ref.at[right])
        send(ref.at[right, 1], ref.at[right, 1], s_sem.at[kind, 4], r_sem.at[kind, 6], left)
        send(ref.at[left], ref.at[left], s_sem.at[kind, 5], r_sem.at[kind, 3], partner)
        send(ref.at[right], ref.at[right], s_sem.at[kind, 6], r_sem.at[kind, 4], partner)
        got(kind, 0, ref.at[partner])

    def across(kind, ref):
        for m in range(2):
            got(kind, 5 + m, ref.at[far, m])
            send(ref.at[far, m], ref.at[far, m], s_sem.at[kind, 7 + m], r_sem.at[kind, 7 + m], partner)
        got(kind, 3, ref.at[p_left])
        got(kind, 4, ref.at[p_right])

    def last(kind, ref):
        for m in range(2):
            got(kind, 7 + m, ref.at[p_far, m])

    own(0, x_all)

    dg = jnp.zeros((1, d), F32)
    for m in range(k):
        _, _, da, db = sides[m]
        for i in range(pieces):
            rows = pl.ds(i * ROWS, ROWS)
            dn = d0[m, rows] + da[1, rows] + db[rows]
            nh = nh_s[m, rows]
            dg = dg + jnp.sum(dn * nh, axis=0, keepdims=True)
            gdn = gf * dn
            dxn = rs_s[m, rows, :1] * (gdn - nh * jnp.mean(nh * gdn, axis=-1, keepdims=True))
            dx_all[me, m, rows] = (dres_ref[m, rows].astype(F32) + dxn).astype(BF16)
    dgs[me] = dg
    own(1, dx_all)
    for o in range(1, n):
        send(dgs.at[me], dgs.at[me], gs_sem.at[o], gr_sem.at[me], (me + o) % n)

    def project(owners, add):
        for p, owner in enumerate(owners):
            for m in range(k):
                base = p * (k * h) + m * h
                du_g[base:base + h] = du_ref[m, pl.ds(pl.multiple_of(owner * h, h), h)]
                for i in range(pieces):
                    xf = x_all[owner, m, pl.ds(i * ROWS, ROWS)].astype(F32)
                    rs = lax.rsqrt(jnp.mean(xf * xf, axis=-1, keepdims=True) + EPS)
                    n_g[base + i * ROWS:base + (i + 1) * ROWS] = ((xf * rs) * gf).astype(BF16)
        u = jnp.dot(n_g[...], w_ref[...], preferred_element_type=F32).astype(BF16)
        for p, owner in enumerate(owners):
            for m in range(k):
                base = p * (k * h) + m * h
                u_ref[m, pl.ds(pl.multiple_of(owner * h, h), h)] = u[base:base + h]
        cw = 512
        for i in range(d // cw):
            v = lax.dot_general(n_g[:, i * cw:(i + 1) * cw], du_g[...], (((0,), (0,)), ((), ())),
                                preferred_element_type=F32)
            rows = slice(i * cw, (i + 1) * cw)
            dw_ref[rows] = dw_ref[rows] + v if add else v

    onward(0, x_all)
    project(near, False)
    onward(1, dx_all)
    across(0, x_all)
    last(0, x_all)
    project(rest, True)
    across(1, dx_all)
    last(1, dx_all)

    for o in range(1, n):
        src = (me + o) % n
        arrived(dgs.at[src], gs_sem.at[o], gr_sem.at[src])
    total_dg = dgs[0]
    for i in range(1, n):
        total_dg = total_dg + dgs[i]
    dg_ref[...] = total_dg
    for c in copies:
        c.wait_send()


def finish(plan, dx_all, x_in, u_in, dw_in, dg_in, de_in, x_ref, u_ref, dw_ref, dg_ref, de_ref, dxf, acc, sem, o_sem):
    del de_in
    outs = [pltpu.make_async_copy(src, dst, o_sem.at[i])
            for i, (src, dst) in enumerate(((dw_in, dw_ref), (u_in, u_ref), (x_in, x_ref)))]
    for c in outs:
        c.start()
    dg_ref[...] = dg_in[...].reshape(dg_ref.shape)
    n, k, h, d = dx_all.shape
    kt = k * h * n

    def widen(i, _):
        for m in range(k):
            for s in range(h // ROWS):
                dxf[pl.ds(pl.multiple_of(i * (k * h) + m * h + s * ROWS, ROWS), ROWS)] = dx_all[i, m, pl.ds(s * ROWS, ROWS)].astype(F32)
        return 0

    lax.fori_loop(0, n, widen, 0)

    sub = lax.broadcasted_iota(jnp.int32, (8, d), 0)
    cnt, used = plan[3 * kt], plan[3 * kt + 1]
    step = 4

    def drain(i, _):
        pltpu.make_async_copy(acc.at[0], de_ref.at[0], sem).wait()
        return 0

    def turn(q, _):
        @pl.when(q > 0)
        def _():
            lax.fori_loop(0, SLOTS, drain, 0)

        def some(b, _):
            todo = []
            for e in range(step):
                i = b * step + e
                c = jnp.minimum(i, cnt - 1)
                code = plan[kt + c]
                s = (code >> 4) - q * SLOTS
                s = jnp.where((i < cnt) & (s >= 0) & (s < SLOTS), s, SLOTS)
                todo.append((s, (code >> 1) & 7, (code & 1) == 1, dxf[pl.ds(plan[c], 1)]))
            for s, r, fresh, x in todo:
                old = jnp.where(fresh, jnp.zeros((8, d), F32), acc[s])
                acc[s] = old + jnp.where(sub == r, jnp.broadcast_to(x, (8, d)), 0.0)
            return 0

        lax.fori_loop(0, lax.div(cnt + step - 1, step), some, 0)

        def put(i, _):
            pltpu.make_async_copy(acc.at[i], de_ref.at[plan[2 * kt + q * SLOTS + i]], sem).start()
            return 0

        lax.fori_loop(0, jnp.minimum(used - q * SLOTS, SLOTS), put, 0)
        return 0

    turns = lax.div(used + SLOTS - 1, SLOTS)
    lax.fori_loop(0, turns, turn, 0)

    for c in outs:
        c.wait()
    lax.fori_loop(0, used - jnp.maximum(turns - 1, 0) * SLOTS, drain, 0)


def solution(mesh):
    n = mesh.shape["tp"]
    chips = n // 2
    to_right = [(r, (r + 2) % n) for r in range(n)]
    to_left = [(r, (r + n - 2) % n) for r in range(n)]
    to_partner = [(r, r ^ 1) for r in range(n)]
    dma = pltpu.SemaphoreType.DMA

    def step(ids, emb, g, w, du, dres):
        k, t = ids.shape
        vl, d = emb.shape
        f = w.shape[1]
        h = t // n
        kt = k * t
        shape = jax.ShapeDtypeStruct
        i32 = lambda *s: shape(s, jnp.int32)
        smem = lambda *s: pltpu.SMEM(s, jnp.int32)
        cost = lambda b: pl.CostEstimate(flops=0, bytes_accessed=b, transcendentals=0)
        limit = lambda mib, **kw: pltpu.CompilerParams(vmem_limit_bytes=mib << 20, **kw)

        def move(v, perm):
            return lax.ppermute(v, "tp", perm)

        flat = shape((kt // 2, d), BF16)
        xm, xo = pl.pallas_call(
            functools.partial(lookup, n),
            out_shape=(flat, flat), in_specs=[SMEM, HBM], out_specs=(VMEM, VMEM),
            scratch_shapes=[pltpu.VMEM((kt, 8, d), BF16), pltpu.VMEM((kt // 8, 8, d), F32), smem(kt + 1), smem(kt), smem(kt), dma],
            compiler_params=limit(32), cost_estimate=cost(16 << 20), name="lookup",
        )(ids, emb.reshape(vl // 8, 8, d))
        xp = move(xo.reshape(chips, k * h, d), to_partner)

        side = shape((chips, k * h, d), BF16)
        dm, do = pl.pallas_call(
            functools.partial(parts, n),
            out_shape=(side, side), in_specs=[VMEM] * 2 + [ANY], out_specs=(VMEM, VMEM),
            scratch_shapes=[pltpu.VMEM((kt, f), BF16)],
            compiler_params=limit(8), cost_estimate=cost(4 << 20), name="parts",
        )(du, w, xm)
        dp = move(do, to_partner)

        def fold_of(a, b, dtype):
            two, one = shape((2, h, d), dtype), shape((h, d), dtype)
            return pl.pallas_call(
                functools.partial(fold, h),
                out_shape=(two, two, one, one, two), in_specs=[VMEM] * 2, out_specs=(VMEM,) * 5,
                compiler_params=limit(8), cost_estimate=cost(2 << 20),
            )(a, b)

        def relay_of(a, b, c, e):
            one = shape(a.shape, a.dtype)
            return pl.pallas_call(
                relay, out_shape=(one, one), in_specs=[VMEM] * 4, out_specs=(VMEM,) * 2,
                compiler_params=limit(8), cost_estimate=cost(2 << 20),
            )(a, b, c, e)

        zr = 16
        unit = vl // 16
        ends = (4 * unit, 10 * unit)
        de_shape = shape((vl // 8, 8, d), F32)
        size = 3 * kt + 128

        def clear_more(de, first, last):
            return pl.pallas_call(
                functools.partial(clear_rest, first, last - first),
                out_shape=de_shape, in_specs=[ANY], out_specs=ANY, input_output_aliases={0: 0},
                scratch_shapes=[pltpu.VMEM((zr, 8, d), F32), dma],
                compiler_params=limit(8), cost_estimate=cost((last - first) * d * 4),
            )(de)

        x_r, x_l, x_n, x_p, x0 = fold_of(xm.reshape(chips, k * h, d), xp, BF16)
        xl1 = move(x_r, to_right)
        xr1 = move(x_l, to_left)
        d_r, d_l, d_n, d_p, d0 = fold_of(dm, dp, F32)
        dl1 = move(d_r, to_right)
        dr1 = move(d_l, to_left)
        de, plan = pl.pallas_call(
            functools.partial(clear_and_list, n, ends[0]),
            out_shape=(de_shape, i32(size)), in_specs=[ANY], out_specs=(ANY, ANY),
            scratch_shapes=[pltpu.VMEM((zr, 8, d), F32), smem(k, t), smem(kt + 1), smem(vl // 8), smem(size),
                            dma, dma((2,))],
            compiler_params=limit(8), cost_estimate=cost(ends[0] * d * 4), name="clear0",
        )(ids)
        x_n, x_p = relay_of(x_n, x_p, xl1, xr1)
        xl2 = move(x_n, to_right)
        xr2 = move(x_p, to_left)
        de = clear_more(de, ends[0], ends[1])
        d_n, d_p = relay_of(d_n, d_p, dl1, dr1)
        dl2 = move(d_n, to_right)
        dr2 = move(d_p, to_left)
        de = clear_more(de, ends[1], vl)

        tok, u_s, dw_s = shape((k, h, d), BF16), shape((k, t, f), BF16), shape((d, f), F32)
        some = kt // 2
        dx_all, x, u, dw, dg = pl.pallas_call(
            functools.partial(spread, n),
            out_shape=(shape((n, k, h, d), BF16), tok, u_s, dw_s, shape((1, d), F32)),
            in_specs=[VMEM] * 14, out_specs=(VMEM,) * 5,
            scratch_shapes=[pltpu.VMEM((n, k, h, d), BF16), pltpu.VMEM((k, h, d), F32), pltpu.VMEM((k, h, 128), F32),
                            pltpu.VMEM((n, 1, d), F32), pltpu.VMEM((some, d), BF16), pltpu.VMEM((some, f), BF16),
                            dma((2, 9)), dma((2, 9)), dma((n,)), dma((n,))],
            compiler_params=limit(24, collective_id=0, has_side_effects=True), name="spread",
        )(x0, xl1, xr1, xl2, xr2, d0, dl1, dr1, dl2, dr2, g, dres, w, du)

        x, u, dw, dg, de = pl.pallas_call(
            finish,
            out_shape=(tok, u_s, dw_s, shape((d,), F32), de_shape),
            in_specs=[SMEM] + [VMEM] * 5 + [ANY], out_specs=(ANY, ANY, ANY, VMEM, ANY),
            input_output_aliases={6: 4},
            scratch_shapes=[pltpu.VMEM((kt, d), F32), pltpu.VMEM((SLOTS + 1, 8, d), F32), dma, dma((3,))],
            compiler_params=limit(24), name="finish",
        )(plan, dx_all, x, u, dw, dg, de)
        return u, x, de.reshape(vl, d), dw, dg

    return jax.shard_map(
        step,
        mesh=mesh,
        in_specs=(P("dp", None), P("tp", None), P(None), P(None, "tp"), P("dp", None, "tp"), P("dp", "tp", None)),
        out_specs=(P("dp", None, "tp"), P("dp", "tp", None), P(("dp", "tp"), None), P(None, ("dp", "tp")), P("dp")),
        check_vma=False,
    )
```

```python
import functools

import jax
import jax.numpy as jnp
from jax import lax
from jax.experimental import pallas as pl
from jax.experimental.pallas import tpu as pltpu
from jax.sharding import PartitionSpec as P


EPS = 1e-6
MESH = pl.DeviceIdType.MESH
VMEM = pl.BlockSpec(memory_space=pltpu.VMEM)
SMEM = pl.BlockSpec(memory_space=pltpu.SMEM)
ANY = pl.BlockSpec(memory_space=pl.ANY)
HBM = pl.BlockSpec(memory_space=pltpu.HBM)
F32 = jnp.float32
BF16 = jnp.bfloat16
ROWS = 16
SLOTS = 128


def slab(i, m, k, h):
    return lax.div(i, h) * (k * h) + m * h + lax.rem(i, h)


def ring_places(n):
    me = lax.axis_index("tp")
    chips = n // 2
    return me, me // 2, me % 2, chips


def parts(n, du_ref, w_ref, after_ref, mine_ref, other_ref, du_g):
    del after_ref
    _, chip, core, chips = ring_places(n)
    k, t, _ = du_ref.shape
    h = t // n
    half = chips * k * h
    for side in range(2):
        for j in range(chips):
            owner = ((chip + j) % chips) * 2 + (core if side == 0 else 1 - core)
            for m in range(k):
                base = side * half + j * (k * h) + m * h
                du_g[base:base + h] = du_ref[m, pl.ds(pl.multiple_of(owner * h, h), h)]
    cw = 256

    def cols(i, _):
        c0 = pl.multiple_of(i * cw, cw)
        v = lax.dot_general(du_g[...], w_ref[pl.ds(c0, cw), :], (((1,), (1,)), ((), ())), preferred_element_type=F32)
        v = v.astype(BF16)
        mine_ref[:, :, pl.ds(c0, cw)] = v[:half].reshape(chips, k * h, cw)
        other_ref[:, :, pl.ds(c0, cw)] = v[half:].reshape(chips, k * h, cw)
        return 0

    lax.fori_loop(0, w_ref.shape[0] // cw, cols, 0)


def lookup(n, ids_ref, emb_ref, mine_ref, other_ref, buf, pf, found, at_s, row_s, sem):
    me, chip, core, chips = ring_places(n)
    k, t = ids_ref.shape
    h = t // n
    d = emb_ref.shape[2]
    vl = emb_ref.shape[0] * 8
    lo = me * vl
    half = chips * k * h

    cnt = jnp.int32(0)
    for m in range(k):
        def find(i, cnt):
            v = ids_ref[m, i]
            found[cnt] = i
            return cnt + ((v >= lo) & (v < lo + vl)).astype(jnp.int32)

        first = cnt
        cnt = lax.fori_loop(0, t, find, first, unroll=16)

        def fetch(c, _):
            i = found[c]
            v = ids_ref[m, i] - lo
            pltpu.make_async_copy(emb_ref.at[lax.div(v, 8)], buf.at[c], sem).start()
            owner = lax.div(i, h)
            side = jnp.where(lax.rem(owner, 2) == core, 0, half)
            j = lax.rem(lax.div(owner, 2) - chip + chips, chips)
            at_s[c] = side + j * (k * h) + m * h + lax.rem(i, h)
            row_s[c] = lax.rem(v, 8)
            return 0

        lax.fori_loop(first, cnt, fetch, 0)

    pf[...] = jnp.zeros_like(pf)
    sub = lax.broadcasted_iota(jnp.int32, (8, d), 0)

    def wait(i, _):
        pltpu.make_async_copy(emb_ref.at[0], buf.at[0], sem).wait()
        return 0

    lax.fori_loop(0, cnt, wait, 0)
    step = 4

    def place(q, _):
        rows = []
        for u in range(step):
            i = jnp.minimum(q * step + u, cnt - 1)
            at = at_s[i]
            to = at & 7
            rows.append((at >> 3, to, pltpu.roll(buf[i].astype(F32), (to - row_s[i]) & 7, 0)))
        for block, to, x in rows:
            pf[block] = jnp.where(sub == to, x, pf[block])
        return 0

    lax.fori_loop(0, lax.div(cnt + step - 1, step), place, 0)

    def pack(i, _):
        r0 = pl.multiple_of(i * ROWS, ROWS)
        b0 = pl.multiple_of(i * (ROWS // 8), ROWS // 8)
        for dst, first in ((mine_ref, 0), (other_ref, half // 8)):
            dst[pl.ds(r0, ROWS)] = pf[pl.ds(first + b0, ROWS // 8)].reshape(ROWS, d).astype(BF16)
        return 0

    lax.fori_loop(0, half // ROWS, pack, 0)


def fold(h, xm, xp, dm, dp, right_ref, left_ref, xn_ref, xv_ref, x0_ref, dn_ref, dv_ref, d0_ref):
    def x(j, m):
        return xm[j, m * h:(m + 1) * h] + xp[j, m * h:(m + 1) * h]

    def dn(j, m):
        return dm[j, m * h:(m + 1) * h].astype(F32) + dp[j, m * h:(m + 1) * h].astype(F32)

    for ref, far, near in ((right_ref, (2, 0), (1, 1)), (left_ref, (2, 1), (3, 0))):
        for i, (j, m) in enumerate((far, near)):
            rows = slice(m * h, (m + 1) * h)
            ref[2 * i] = dm[j, rows]
            ref[2 * i + 1] = dp[j, rows]
            ref[4 + i] = x(j, m)
    xn_ref[...] = x(1, 0)
    xv_ref[...] = x(3, 1)
    dn_ref[...] = dn(1, 0)
    dv_ref[...] = dn(3, 1)
    for m in range(2):
        x0_ref[m] = x(0, m)
        d0_ref[m] = dn(0, m)


def relay(xn, xv, dn, dv, fl, fr, xn_ref, xv_ref, dn_ref, dv_ref):
    dn_ref[...] = dn[...] + fl[0].astype(F32) + fl[1].astype(F32)
    dv_ref[...] = dv[...] + fr[0].astype(F32) + fr[1].astype(F32)
    xn_ref[...] = xn[...] + fl[4]
    xv_ref[...] = xv[...] + fr[4]


def zeros(z, de_ref, first, rows, sem):
    zr = z.shape[0]
    z[...] = jnp.zeros_like(z)
    cs = [pltpu.make_async_copy(z, de_ref.at[pl.ds(first // 8 + i * zr, zr)], sem) for i in range(rows // (8 * zr))]
    for c in cs:
        c.start()
    return cs


def clear_and_list(n, rows, ids_hbm, de_ref, plan_ref, z, ids, found, table, plan, sem, s_sem):
    load = pltpu.make_async_copy(ids_hbm, ids, s_sem.at[0])
    load.start()
    cs = zeros(z, de_ref, 0, rows, sem)
    k, t = ids.shape
    h, kt = t // n, k * t
    vl = de_ref.shape[0] * 8
    lo = lax.axis_index("tp") * vl

    def reset(i, _):
        table[i] = -1
        return 0

    lax.fori_loop(0, table.shape[0], reset, 0, unroll=8)
    load.wait()
    cnt, used = jnp.int32(0), jnp.int32(0)
    for m in range(k):
        def find(i, cnt):
            v = ids[m, i]
            found[cnt] = i
            return cnt + ((v >= lo) & (v < lo + vl)).astype(jnp.int32)

        first = cnt
        cnt = lax.fori_loop(0, t, find, first, unroll=16)

        def one(c, used):
            i = found[c]
            v = ids[m, i] - lo
            b = lax.div(v, 8)
            s = table[b]
            fresh = (s < 0).astype(jnp.int32)
            s = jnp.where(s < 0, used, s)
            table[b] = s
            plan[c] = slab(i, m, k, h)
            plan[kt + c] = s * 16 + lax.rem(v, 8) * 2 + fresh
            plan[2 * kt + s] = b
            return used + fresh

        used = lax.fori_loop(first, cnt, one, used)
    plan[3 * kt] = cnt
    plan[3 * kt + 1] = used
    store = pltpu.make_async_copy(plan, plan_ref, s_sem.at[1])
    store.start()
    store.wait()
    for c in cs:
        c.wait()


def clear_rest(first, rows, de_in, de_ref, z, sem):
    del de_in
    for c in zeros(z, de_ref, first, rows, sem):
        c.wait()


def spread(n, fl, fr, x0, xl2, xr2, d0, dl2, dr2, g_ref, dres_ref, w_ref, du_ref,
           dx_all, x_ref, u_ref, dw_ref, dg_ref, x_all, nh_s, rs_s, dgs, n_g, du_g, s_sem, r_sem, gs_sem, gr_sem):
    me, chip, core, chips = ring_places(n)
    k, h, d = dres_ref.shape
    at = lambda off, c: ((chip + off) % chips) * 2 + c
    left, right, far = at(chips - 1, core), at(1, core), at(2, core)
    partner, p_left, p_right, p_far = at(0, 1 - core), at(chips - 1, 1 - core), at(1, 1 - core), at(2, 1 - core)
    early = (me, left, right, partner, p_left, p_right)
    late = (far, p_far)

    barrier = pltpu.get_barrier_semaphore()
    for o in range(1, n):
        pl.semaphore_signal(barrier, inc=1, device_id={"tp": (me + o) % n}, device_id_type=MESH)

    gf = g_ref[...].astype(F32).reshape(1, d)
    pieces = h // ROWS
    sides = ((fr, xl2, dl2), (fl, xr2, dr2))
    for m in range(k):
        one, xb, _ = sides[m]
        for i in range(pieces):
            rows = pl.ds(i * ROWS, ROWS)
            x = x0[m, rows] + one[5, rows] + xb[rows]
            x_ref[m, rows] = x
            x_all[me, m, rows] = x
            xf = x.astype(F32)
            rs = lax.rsqrt(jnp.mean(xf * xf, axis=-1, keepdims=True) + EPS)
            nh_s[m, rows] = xf * rs
            rs_s[m, rows] = jnp.broadcast_to(rs, (ROWS, rs_s.shape[-1]))
    pl.semaphore_wait(barrier, n - 1)

    copies = []

    def send(src, dst, ss, rs, to):
        c = pltpu.make_async_remote_copy(src_ref=src, dst_ref=dst, send_sem=ss, recv_sem=rs,
                                         device_id={"tp": to}, device_id_type=MESH)
        c.start()
        copies.append(c)

    def arrived(dst, ss, rs):
        pltpu.make_async_remote_copy(src_ref=dst, dst_ref=dst, send_sem=ss, recv_sem=rs,
                                     device_id={"tp": partner}, device_id_type=MESH).wait_recv()

    def own(kind, ref):
        for slot, (to, rel) in enumerate(((right, 1), (left, 2), (partner, 0))):
            send(ref.at[me], ref.at[me], s_sem.at[kind, slot], r_sem.at[kind, rel], to)

    def got(kind, rel, view):
        arrived(view, s_sem.at[kind, rel], r_sem.at[kind, rel])

    def onward(kind, ref):
        got(kind, 1, ref.at[left])
        send(ref.at[left, 0], ref.at[left, 0], s_sem.at[kind, 3], r_sem.at[kind, 5], right)
        got(kind, 2, ref.at[right])
        send(ref.at[right, 1], ref.at[right, 1], s_sem.at[kind, 4], r_sem.at[kind, 6], left)
        send(ref.at[left], ref.at[left], s_sem.at[kind, 5], r_sem.at[kind, 3], partner)
        send(ref.at[right], ref.at[right], s_sem.at[kind, 6], r_sem.at[kind, 4], partner)
        got(kind, 0, ref.at[partner])
        got(kind, 3, ref.at[p_left])
        got(kind, 4, ref.at[p_right])

    def across(kind, ref):
        for m in range(2):
            got(kind, 5 + m, ref.at[far, m])
            send(ref.at[far, m], ref.at[far, m], s_sem.at[kind, 7 + m], r_sem.at[kind, 7 + m], partner)

    def last(kind, ref):
        for m in range(2):
            got(kind, 7 + m, ref.at[p_far, m])

    own(0, x_all)

    dg = jnp.zeros((1, d), F32)
    for m in range(k):
        one, _, db = sides[m]
        for i in range(pieces):
            rows = pl.ds(i * ROWS, ROWS)
            dn = d0[m, rows] + one[2, rows].astype(F32) + one[3, rows].astype(F32) + db[rows]
            nh = nh_s[m, rows]
            dg = dg + jnp.sum(dn * nh, axis=0, keepdims=True)
            gdn = gf * dn
            dxn = rs_s[m, rows, :1] * (gdn - nh * jnp.mean(nh * gdn, axis=-1, keepdims=True))
            dx_all[me, m, rows] = (dres_ref[m, rows].astype(F32) + dxn).astype(BF16)
    dgs[me] = dg
    own(1, dx_all)
    for o in range(1, n):
        send(dgs.at[me], dgs.at[me], gs_sem.at[o], gr_sem.at[me], (me + o) % n)

    def project(owners, add):
        for p, owner in enumerate(owners):
            for m in range(k):
                base = p * (k * h) + m * h
                du_g[base:base + h] = du_ref[m, pl.ds(pl.multiple_of(owner * h, h), h)]
                for i in range(pieces):
                    xf = x_all[owner, m, pl.ds(i * ROWS, ROWS)].astype(F32)
                    rs = lax.rsqrt(jnp.mean(xf * xf, axis=-1, keepdims=True) + EPS)
                    n_g[base + i * ROWS:base + (i + 1) * ROWS] = ((xf * rs) * gf).astype(BF16)
        size = len(owners) * k * h
        u = jnp.dot(n_g[:size], w_ref[...], preferred_element_type=F32).astype(BF16)
        for p, owner in enumerate(owners):
            for m in range(k):
                base = p * (k * h) + m * h
                u_ref[m, pl.ds(pl.multiple_of(owner * h, h), h)] = u[base:base + h]
        cw = 512
        for i in range(d // cw):
            v = lax.dot_general(n_g[:size, i * cw:(i + 1) * cw], du_g[:size], (((0,), (0,)), ((), ())),
                                preferred_element_type=F32)
            rows = slice(i * cw, (i + 1) * cw)
            dw_ref[rows] = dw_ref[rows] + v if add else v

    onward(0, x_all)
    project(early, False)
    onward(1, dx_all)
    across(0, x_all)
    last(0, x_all)
    project(late, True)
    across(1, dx_all)
    last(1, dx_all)

    for o in range(1, n):
        src = (me + o) % n
        arrived(dgs.at[src], gs_sem.at[o], gr_sem.at[src])
    total_dg = dgs[0]
    for i in range(1, n):
        total_dg = total_dg + dgs[i]
    dg_ref[...] = total_dg
    for c in copies:
        c.wait_send()


def finish(plan, dx_all, x_in, u_in, dw_in, dg_in, de_in, x_ref, u_ref, dw_ref, dg_ref, de_ref, dxf, acc, sem, o_sem):
    del de_in
    outs = [pltpu.make_async_copy(src, dst, o_sem.at[i])
            for i, (src, dst) in enumerate(((dw_in, dw_ref), (u_in, u_ref), (x_in, x_ref)))]
    for c in outs:
        c.start()
    dg_ref[...] = dg_in[...].reshape(dg_ref.shape)
    n, k, h, d = dx_all.shape
    kt = k * h * n

    def widen(i, _):
        for m in range(k):
            for s in range(h // ROWS):
                dxf[pl.ds(pl.multiple_of(i * (k * h) + m * h + s * ROWS, ROWS), ROWS)] = dx_all[i, m, pl.ds(s * ROWS, ROWS)].astype(F32)
        return 0

    lax.fori_loop(0, n, widen, 0)

    sub = lax.broadcasted_iota(jnp.int32, (8, d), 0)
    cnt, used = plan[3 * kt], plan[3 * kt + 1]
    step = 4

    def drain(i, _):
        pltpu.make_async_copy(acc.at[0], de_ref.at[0], sem).wait()
        return 0

    def turn(q, _):
        @pl.when(q > 0)
        def _():
            lax.fori_loop(0, SLOTS, drain, 0)

        def some(b, _):
            todo = []
            for e in range(step):
                i = b * step + e
                c = jnp.minimum(i, cnt - 1)
                code = plan[kt + c]
                s = (code >> 4) - q * SLOTS
                s = jnp.where((i < cnt) & (s >= 0) & (s < SLOTS), s, SLOTS)
                todo.append((s, (code >> 1) & 7, (code & 1) == 1, dxf[pl.ds(plan[c], 1)]))
            for s, r, fresh, x in todo:
                old = jnp.where(fresh, jnp.zeros((8, d), F32), acc[s])
                acc[s] = old + jnp.where(sub == r, jnp.broadcast_to(x, (8, d)), 0.0)
            return 0

        lax.fori_loop(0, lax.div(cnt + step - 1, step), some, 0)

        def put(i, _):
            pltpu.make_async_copy(acc.at[i], de_ref.at[plan[2 * kt + q * SLOTS + i]], sem).start()
            return 0

        lax.fori_loop(0, jnp.minimum(used - q * SLOTS, SLOTS), put, 0)
        return 0

    turns = lax.div(used + SLOTS - 1, SLOTS)
    lax.fori_loop(0, turns, turn, 0)

    for c in outs:
        c.wait()
    lax.fori_loop(0, used - jnp.maximum(turns - 1, 0) * SLOTS, drain, 0)


def solution(mesh):
    n = mesh.shape["tp"]
    chips = n // 2
    to_right = [(r, (r + 2) % n) for r in range(n)]
    to_left = [(r, (r + n - 2) % n) for r in range(n)]
    to_partner = [(r, r ^ 1) for r in range(n)]
    dma = pltpu.SemaphoreType.DMA

    def step(ids, emb, g, w, du, dres):
        k, t = ids.shape
        vl, d = emb.shape
        f = w.shape[1]
        h = t // n
        kt = k * t
        shape = jax.ShapeDtypeStruct
        i32 = lambda *s: shape(s, jnp.int32)
        smem = lambda *s: pltpu.SMEM(s, jnp.int32)
        cost = lambda b: pl.CostEstimate(flops=0, bytes_accessed=b, transcendentals=0)
        limit = lambda mib, **kw: pltpu.CompilerParams(vmem_limit_bytes=mib << 20, **kw)

        def move(v, perm):
            return lax.ppermute(v, "tp", perm)

        flat = shape((kt // 2, d), BF16)
        xm, xo = pl.pallas_call(
            functools.partial(lookup, n),
            out_shape=(flat, flat), in_specs=[SMEM, HBM], out_specs=(VMEM, VMEM),
            scratch_shapes=[pltpu.VMEM((kt, 8, d), BF16), pltpu.VMEM((kt // 8, 8, d), F32), smem(kt + 1), smem(kt), smem(kt), dma],
            compiler_params=limit(32), cost_estimate=cost(16 << 20), name="lookup",
        )(ids, emb.reshape(vl // 8, 8, d))
        xp = move(xo.reshape(chips, k * h, d), to_partner)

        side = shape((chips, k * h, d), BF16)
        dm, do = pl.pallas_call(
            functools.partial(parts, n),
            out_shape=(side, side), in_specs=[VMEM] * 2 + [ANY], out_specs=(VMEM, VMEM),
            scratch_shapes=[pltpu.VMEM((kt, f), BF16)],
            compiler_params=limit(8), cost_estimate=cost(4 << 20), name="parts",
        )(du, w, xm)
        dp = move(do, to_partner)

        zr = 16
        unit = vl // 16
        split = 13 * unit
        de_shape = shape((vl // 8, 8, d), F32)
        size = 3 * kt + 128

        chunk, half_x, half_d = shape((6, h, d), BF16), shape((h, d), BF16), shape((h, d), F32)
        to_r, to_l, x_n, x_v, x0, d_n, d_v, d0 = pl.pallas_call(
            functools.partial(fold, h),
            out_shape=(chunk, chunk, half_x, half_x, shape((2, h, d), BF16), half_d, half_d, shape((2, h, d), F32)),
            in_specs=[VMEM] * 4, out_specs=(VMEM,) * 8,
            compiler_params=limit(8), cost_estimate=cost(4 << 20), name="fold",
        )(xm.reshape(chips, k * h, d), xp, dm, dp)
        fl = move(to_r, to_right)
        fr = move(to_l, to_left)
        de, plan = pl.pallas_call(
            functools.partial(clear_and_list, n, split),
            out_shape=(de_shape, i32(size)), in_specs=[ANY], out_specs=(ANY, ANY),
            scratch_shapes=[pltpu.VMEM((zr, 8, d), F32), smem(k, t), smem(kt + 1), smem(vl // 8), smem(size),
                            dma, dma((2,))],
            compiler_params=limit(8), cost_estimate=cost(split * d * 4), name="clear0",
        )(ids)
        x_n, x_v, d_n, d_v = pl.pallas_call(
            relay, out_shape=(half_x, half_x, half_d, half_d), in_specs=[VMEM] * 6, out_specs=(VMEM,) * 4,
            compiler_params=limit(8), cost_estimate=cost(2 << 20), name="relay",
        )(x_n, x_v, d_n, d_v, fl, fr)
        dl2 = move(d_n, to_right)
        dr2 = move(d_v, to_left)
        xl2 = move(x_n, to_right)
        xr2 = move(x_v, to_left)
        de = pl.pallas_call(
            functools.partial(clear_rest, split, vl - split),
            out_shape=de_shape, in_specs=[ANY], out_specs=ANY, input_output_aliases={0: 0},
            scratch_shapes=[pltpu.VMEM((zr, 8, d), F32), dma],
            compiler_params=limit(8), cost_estimate=cost((vl - split) * d * 4), name="clear1",
        )(de)

        tok, u_s, dw_s = shape((k, h, d), BF16), shape((k, t, f), BF16), shape((d, f), F32)
        some = 6 * k * h
        dx_all, x, u, dw, dg = pl.pallas_call(
            functools.partial(spread, n),
            out_shape=(shape((n, k, h, d), BF16), tok, u_s, dw_s, shape((1, d), F32)),
            in_specs=[VMEM] * 12, out_specs=(VMEM,) * 5,
            scratch_shapes=[pltpu.VMEM((n, k, h, d), BF16), pltpu.VMEM((k, h, d), F32), pltpu.VMEM((k, h, 128), F32),
                            pltpu.VMEM((n, 1, d), F32), pltpu.VMEM((some, d), BF16), pltpu.VMEM((some, f), BF16),
                            dma((2, 9)), dma((2, 9)), dma((n,)), dma((n,))],
            compiler_params=limit(24, collective_id=0, has_side_effects=True), name="spread",
        )(fl, fr, x0, xl2, xr2, d0, dl2, dr2, g, dres, w, du)

        x, u, dw, dg, de = pl.pallas_call(
            finish,
            out_shape=(tok, u_s, dw_s, shape((d,), F32), de_shape),
            in_specs=[SMEM] + [VMEM] * 5 + [ANY], out_specs=(ANY, ANY, ANY, VMEM, ANY),
            input_output_aliases={6: 4},
            scratch_shapes=[pltpu.VMEM((kt, d), F32), pltpu.VMEM((SLOTS + 1, 8, d), F32), dma, dma((3,))],
            compiler_params=limit(24), name="finish",
        )(plan, dx_all, x, u, dw, dg, de)
        return u, x, de.reshape(vl, d), dw, dg

    return jax.shard_map(
        step,
        mesh=mesh,
        in_specs=(P("dp", None), P("tp", None), P(None), P(None, "tp"), P("dp", None, "tp"), P("dp", "tp", None)),
        out_specs=(P("dp", None, "tp"), P("dp", "tp", None), P(("dp", "tp"), None), P(None, ("dp", "tp")), P("dp")),
        check_vma=False,
    )
```
